32 devices in a mesh: groups: 2 (over y), dom: 8 (over z, core), tilt: 2 (over x), rep: 1.
Axes of the slice: x: 2, y: 2, z: 4, core: 2. Of those that a mesh axis runs over, the one named last changes fastest.
Arguments:
- patches: bfloat16 [4, 1024, 128, 128], P(('groups', 'tilt'), 'dom'), parts along dimension 0, may hold values from -6 to 6
- slot_view: int32 [4, 1024, 1], P(('groups', 'tilt'), 'dom'), parts along dimension 0, may hold values from 0 to 31, as said below
- slot_tilt: int32 [4, 1024], P(('groups', 'tilt'), 'dom'), parts along dimension 0, may hold values from 0 to 9
- slot_pos: bfloat16 [2, 4, 1024], P(None, ('groups', 'tilt'), 'dom'), parts along dimension 1, may hold values from 0 to 1
- defocus: bfloat16 [4, 1024], P(('groups', 'tilt'), 'dom'), parts along dimension 0, may hold values from 1 to 3
- projections: bfloat16 [64, 20, 2, 128, 128], P(('groups', 'dom'), 'tilt', None, 'rep'), parts along dimension 0, may hold values from -6 to 6
- warp_grid: float32 [40, 2, 256], P(('groups', 'tilt')), parts along dimension 0, may hold values from -6 to 6
Outputs:
- slot_terms: float32 [3, 4, 1024], P(None, ('groups', 'tilt'), 'dom'), parts along dimension 1
- new_warp: float32 [40, 2, 256], P(('groups', 'tilt')), parts along dimension 0
The draws below stay inside these ranges and needn't reach their ends.
There are 2 independent parts, one for each index of `groups`. The reference program is written for one: setup_inputs(seed, part) draws one part's arguments, and reference() takes and returns one part's arrays. A program takes and returns all parts, laid end to end along the dimension named above; each array names one. Nothing has to cross between parts.
Inputs may be any that keep to these rules, and one draw needn't show every extreme that they name: `slot_view`: view v is owned by dom index v // 4. Among the 128 slots of one device (one tilt index and one dom index) at most 24 name views of any one owner, and in every such block some owner is named exactly 24 times.
All inputs are finite; a program needn't handle non-finite values.
Results may differ from the reference program's by a relative error of at most 0.0018.
Values may be sent and summed in bfloat16 or wider, within the bound.
A program may use at most 64 MiB of HBM per device.

```python
import math
import jax
import jax.numpy as jnp
from jax import lax

PATCH = 128
GRID = 16
VIEW_DEV = 4
TILT_DEV = 10
SLOT_DEV = 128
VIEWS = 32
TILTS = 20
SLOTS = 1024
OWN_CAP = 24
NODES = 256
N_DOM = 8
N_TILT = 2


def draw_slot_view(key, part):
    block_total = N_TILT * N_DOM
    base_load = SLOT_DEV // N_DOM
    spare_load = OWN_CAP - base_load
    half_owners = N_DOM // 2
    hot_owner = jax.random.randint(jax.random.fold_in(key, 7), (), 0, N_DOM).astype(jnp.int32)

    def one_block(block_key):
        key_order, key_delta, key_shuffle, key_view = jax.random.split(block_key, 4)
        order = jax.random.permutation(key_order, N_DOM - 1).astype(jnp.int32)
        others = order + (order >= hot_owner).astype(jnp.int32)
        arrange = jnp.concatenate([hot_owner[None], others])
        delta = jax.random.randint(key_delta, (half_owners,), 0, spare_load + 1).astype(jnp.int32)
        delta = delta.at[0].set(spare_load)
        deltas = jnp.concatenate([delta, -delta])
        counts = jnp.zeros((N_DOM,), jnp.int32).at[arrange].set(base_load + deltas)
        ends = jnp.cumsum(counts)
        slot_iota = jnp.arange(SLOT_DEV, dtype=jnp.int32)
        owner = jnp.sum((ends[None, :] <= slot_iota[:, None]).astype(jnp.int32), axis=1)
        owner = owner[jax.random.permutation(key_shuffle, SLOT_DEV)]
        return owner * VIEW_DEV + jax.random.randint(key_view, (SLOT_DEV,), 0, VIEW_DEV).astype(jnp.int32)
    block_keys = jax.random.split(jax.random.fold_in(key, 3), block_total)
    views_all = jax.vmap(one_block)(block_keys)
    return views_all.reshape(N_TILT, SLOTS, 1).astype(jnp.int32)


def place_ends(array, stream_key, least, largest):
    longest = array.shape.index(max(array.shape))
    spots = []
    for shift in (0, 1):
        where = [jax.random.randint(jax.random.fold_in(stream_key, axis), (), 0, length) for axis, length in enumerate(array.shape)]
        where[longest] = (where[longest] + shift) % array.shape[longest]
        spots.append(tuple(where))
    return array.at[spots[0]].set(least).at[spots[1]].set(largest)


def levels(stream_key, extent, cuts, low, largest):
    def one(dim, parts):
        steps = jax.random.uniform(jax.random.fold_in(jax.random.fold_in(stream_key, 6), dim), (parts,), jnp.float32, low / len(cuts), largest / len(cuts))
        return jnp.repeat(jnp.exp(steps), extent[dim] // parts).reshape((-1,) + (1,) * (len(extent) - dim - 1))

    loudness = one(*cuts[0])
    for cut in cuts[1:]:
        loudness = loudness * one(*cut)
    return loudness


def gaussian(own_key, extent, scale, limit, shards=(), held_as=jnp.bfloat16):
    values = scale * jax.random.normal(own_key, extent, jnp.float32)
    if shards:
        values = values * levels(own_key, extent, shards, -0.22, 0.18)
    return jnp.clip(values, -limit, limit).astype(held_as)


def setup_inputs(seed: int = 0, part: int = 0) -> dict:
    splits = jax.random.split(jax.random.key(seed), 8)
    part_splits = jax.random.split(jax.random.fold_in(splits[7], part), 8)
    return {
        "patches": gaussian(part_splits[0], (N_TILT, SLOTS, PATCH, PATCH), 1.0, 6.0, ((0, 2), (1, 8))),
        "slot_view": draw_slot_view(jax.random.fold_in(jax.random.fold_in(splits[7], part), 71), part),
        "slot_tilt": place_ends(jax.random.randint(part_splits[2], (N_TILT, SLOTS), 0, TILT_DEV), jax.random.fold_in(part_splits[2], 1), 0, TILT_DEV - 1).astype(jnp.int32),
        "slot_pos": jnp.clip(1.0 * jax.random.uniform(part_splits[3], (2, N_TILT, SLOTS), jnp.float32) ** levels(part_splits[3], (2, N_TILT, SLOTS), ((1, 2), (2, 8)), -0.2, 0.2), 0.0, 1.0).astype(jnp.bfloat16),
        "defocus": jnp.clip(jnp.exp(math.log(3.0) - 1.0986123 * jax.random.uniform(part_splits[4], (N_TILT, SLOTS), jnp.float32) ** levels(part_splits[4], (N_TILT, SLOTS), ((0, 2), (1, 8)), -0.2, 0.2)), 1.0, 3.0).astype(jnp.bfloat16),
        "projections": gaussian(part_splits[5], (VIEWS, TILTS, 2, PATCH, PATCH), 1.0, 6.0, ((0, 8), (1, 2))),
        "warp_grid": gaussian(part_splits[6], (TILTS, 2, NODES), 1.5, 6.0, ((0, 2),), jnp.float32),
    }


AMPLITUDE = 0.07
TRUST_FLOOR = 0.02

def signed_freq(index, pixels):
    return jnp.where(index < pixels // 2, index, index - pixels).astype(jnp.float32)

def dft_tables(freq_rows, pixels):
    columns = jnp.arange(pixels, dtype=jnp.int32)
    table_scale = 1.0 / math.sqrt(pixels)
    turns_rows = (freq_rows[:, None] * columns[None, :] % pixels).astype(jnp.float32) * (2.0 * math.pi / pixels)
    turns_full = (columns[:, None] * columns[None, :] % pixels).astype(jnp.float32) * (2.0 * math.pi / pixels)
    row_table = jnp.concatenate([jnp.cos(turns_rows), jnp.sin(turns_rows)], axis=0) * table_scale
    col_table = jnp.concatenate([jnp.cos(turns_full), jnp.sin(turns_full)], axis=1) * table_scale
    return (row_table.astype(jnp.bfloat16), col_table.astype(jnp.bfloat16))

def node_weights(pos_x, pos_y, grid_side):
    knot_pos = jnp.arange(grid_side, dtype=jnp.int32).astype(jnp.float32)
    weight_x = jnp.maximum(0.0, 1.0 - jnp.abs(pos_x[:, None] * (grid_side - 1) - knot_pos[None, :]))
    weight_y = jnp.maximum(0.0, 1.0 - jnp.abs(pos_y[:, None] * (grid_side - 1) - knot_pos[None, :]))
    return (weight_y[:, :, None] * weight_x[:, None, :]).reshape(pos_x.shape[0], grid_side * grid_side)

def spectral_terms(spectrum, ref_blk, focus_blk, shift_blk, freq_rows, pixels):
    row_total = freq_rows.shape[0]
    v_one_cos = spectrum[:, :row_total, :pixels]
    v_one_sin = spectrum[:, :row_total, pixels:]
    v_two_cos = spectrum[:, row_total:, :pixels]
    v_two_sin = spectrum[:, row_total:, pixels:]
    real_part = v_one_cos - v_two_sin
    imag_part = -(v_one_sin + v_two_cos)
    freq_y = signed_freq(freq_rows, pixels)[None, :, None]
    freq_x = signed_freq(jnp.arange(pixels, dtype=jnp.int32), pixels)[None, None, :]
    nyquist = pixels / 2.0
    radius = (freq_y * freq_y + freq_x * freq_x) / (nyquist * nyquist)
    aberration = math.pi * focus_blk[:, None, None] * radius
    contrast = -(math.sqrt(1.0 - AMPLITUDE * AMPLITUDE) * jnp.sin(aberration) + AMPLITUDE * jnp.cos(aberration))
    phase_angle = 2.0 * math.pi / pixels * (freq_x * shift_blk[:, 0, None, None] + freq_y * shift_blk[:, 1, None, None])
    cosine = jnp.cos(phase_angle)
    sine_part = jnp.sin(phase_angle)
    ref_real = ref_blk[:, 0].astype(jnp.float32)
    ref_imag = ref_blk[:, 1].astype(jnp.float32)
    model_real = contrast * (ref_real * cosine + ref_imag * sine_part)
    model_imag = contrast * (ref_imag * cosine - ref_real * sine_part)
    diff_real = real_part - model_real
    diff_imag = imag_part - model_imag
    inverse_area = 1.0 / (pixels * pixels)
    energy = lax.optimization_barrier(jnp.sum(diff_real * diff_real + diff_imag * diff_imag, axis=(1, 2))) * inverse_area
    cross_term = diff_imag * model_real - diff_real * model_imag
    grad_x = 2.0 * inverse_area * lax.optimization_barrier(jnp.sum(2.0 * math.pi / pixels * freq_x * cross_term, axis=(1, 2)))
    grad_y = 2.0 * inverse_area * lax.optimization_barrier(jnp.sum(2.0 * math.pi / pixels * freq_y * cross_term, axis=(1, 2)))
    return jnp.stack([energy, grad_x, grad_y], axis=1)

def reference(patches, slot_view, slot_tilt, slot_pos, defocus, projections, warp_grid):
    slot_total = N_TILT * SLOTS
    tilt_index = (jnp.arange(N_TILT, dtype=jnp.int32)[:, None] * TILT_DEV + slot_tilt).reshape(slot_total).astype(jnp.int32)
    view_index = slot_view.reshape(slot_total).astype(jnp.int32)
    weights = node_weights(slot_pos[0].reshape(slot_total).astype(jnp.float32), slot_pos[1].reshape(slot_total).astype(jnp.float32), GRID)
    shifts = lax.optimization_barrier(jnp.sum(warp_grid[tilt_index] * weights[:, None, :], axis=2))
    focus = defocus.reshape(slot_total).astype(jnp.float32)
    freq_rows = jnp.arange(PATCH, dtype=jnp.int32)
    row_table, col_table = dft_tables(freq_rows, PATCH)
    block_len = math.gcd(slot_total, 32)
    block_count = slot_total // block_len

    def one_block(inputs):
        patch_blk, view_blk, tilt_blk, focus_blk, shift_blk = inputs
        ref_blk = projections[view_blk, tilt_blk]
        first_pass = jnp.einsum('fy,byx->bfx', row_table.astype(jnp.float32), patch_blk.astype(jnp.float32)).astype(jnp.bfloat16)
        spectrum = jnp.einsum('bfx,xk->bfk', first_pass.astype(jnp.float32), col_table.astype(jnp.float32))
        return spectral_terms(spectrum, ref_blk, focus_blk, shift_blk, freq_rows, PATCH)
    per_slot = lax.map(one_block, (patches.reshape(block_count, block_len, PATCH, PATCH), view_index.reshape(block_count, block_len), tilt_index.reshape(block_count, block_len), focus.reshape(block_count, block_len), shifts.reshape(block_count, block_len, 2))).reshape(slot_total, 3)
    slot_terms = per_slot.T.reshape(3, N_TILT, SLOTS)
    tilt_hits = (tilt_index[:, None] == jnp.arange(TILTS, dtype=jnp.int32)[None, :]).astype(jnp.float32)
    node_coef = (tilt_hits[:, :, None] * per_slot[:, None, 1:3]).reshape(slot_total, 2 * TILTS)
    gradient = jnp.dot(node_coef.T, weights, precision=lax.Precision.HIGHEST, preferred_element_type=jnp.float32).reshape(TILTS, 2, NODES)
    new_warp = warp_grid - gradient / jnp.sqrt(gradient * gradient + TRUST_FLOOR * TRUST_FLOOR)
    return (slot_terms, new_warp)
```

```python
import functools
import math

import jax
import jax.numpy as jnp
from jax import lax
from jax.experimental import pallas as pl
from jax.experimental.pallas import tpu as pltpu
from jax.sharding import PartitionSpec as P

GRID = 16


AMPLITUDE = 0.07
TRUST_FLOOR = 0.02


def signed_freq(index, pixels):
    return jnp.where(index < pixels // 2, index, index - pixels).astype(jnp.float32)


def dft_tables(freq_rows, pixels):
    columns = jnp.arange(pixels, dtype=jnp.int32)
    table_scale = 1.0 / math.sqrt(pixels)
    turns_rows = (freq_rows[:, None] * columns[None, :] % pixels).astype(jnp.float32) * (
        2.0 * math.pi / pixels
    )
    turns_full = (columns[:, None] * columns[None, :] % pixels).astype(jnp.float32) * (
        2.0 * math.pi / pixels
    )
    row_table = jnp.concatenate([jnp.cos(turns_rows), jnp.sin(turns_rows)], axis=0) * table_scale
    col_table = jnp.concatenate([jnp.cos(turns_full), jnp.sin(turns_full)], axis=1) * table_scale
    return (row_table.astype(jnp.bfloat16), col_table.astype(jnp.bfloat16))


def node_weights(pos_x, pos_y, grid_side):
    knot_pos = jnp.arange(grid_side, dtype=jnp.int32).astype(jnp.float32)
    weight_x = jnp.maximum(0.0, 1.0 - jnp.abs(pos_x[:, None] * (grid_side - 1) - knot_pos[None, :]))
    weight_y = jnp.maximum(0.0, 1.0 - jnp.abs(pos_y[:, None] * (grid_side - 1) - knot_pos[None, :]))
    return (weight_y[:, :, None] * weight_x[:, None, :]).reshape(
        pos_x.shape[0], grid_side * grid_side
    )


def spectral_terms(spectrum, ref_blk, focus_blk, shift_blk, freq_rows, pixels):
    row_total = freq_rows.shape[0]
    v_one_cos = spectrum[:, :row_total, :pixels]
    v_one_sin = spectrum[:, :row_total, pixels:]
    v_two_cos = spectrum[:, row_total:, :pixels]
    v_two_sin = spectrum[:, row_total:, pixels:]
    real_part = v_one_cos - v_two_sin
    imag_part = -(v_one_sin + v_two_cos)
    freq_y = signed_freq(freq_rows, pixels)[None, :, None]
    freq_x = signed_freq(jnp.arange(pixels, dtype=jnp.int32), pixels)[None, None, :]
    nyquist = pixels / 2.0
    radius = (freq_y * freq_y + freq_x * freq_x) / (nyquist * nyquist)
    aberration = math.pi * focus_blk[:, None, None] * radius
    contrast = -(
        math.sqrt(1.0 - AMPLITUDE * AMPLITUDE) * jnp.sin(aberration)
        + AMPLITUDE * jnp.cos(aberration)
    )
    phase_angle = (
        2.0
        * math.pi
        / pixels
        * (freq_x * shift_blk[:, 0, None, None] + freq_y * shift_blk[:, 1, None, None])
    )
    cosine = jnp.cos(phase_angle)
    sine_part = jnp.sin(phase_angle)
    ref_real = ref_blk[:, 0].astype(jnp.float32)
    ref_imag = ref_blk[:, 1].astype(jnp.float32)
    model_real = contrast * (ref_real * cosine + ref_imag * sine_part)
    model_imag = contrast * (ref_imag * cosine - ref_real * sine_part)
    diff_real = real_part - model_real
    diff_imag = imag_part - model_imag
    inverse_area = 1.0 / (pixels * pixels)
    energy = jnp.sum(diff_real * diff_real + diff_imag * diff_imag, axis=(1, 2)) * inverse_area
    cross_term = diff_imag * model_real - diff_real * model_imag
    grad_x = 2.0 * inverse_area * jnp.sum(2.0 * math.pi / pixels * freq_x * cross_term, axis=(1, 2))
    grad_y = 2.0 * inverse_area * jnp.sum(2.0 * math.pi / pixels * freq_y * cross_term, axis=(1, 2))
    return jnp.stack([energy, grad_x, grad_y], axis=1)


def on_device(patches, slot_view, slot_tilt, slot_pos, defocus, projections, warp_grid):
    owners = lax.axis_size("dom")
    slot_count = patches.shape[1]
    pixels = patches.shape[-1]
    view_dev = projections.shape[0]
    tilt_dev = warp_grid.shape[0]
    node_count = warp_grid.shape[2]
    capacity = 3 * slot_count // (2 * owners)
    buffer_len = owners * capacity
    chosen_view = slot_view[0, :, 0]
    owner_of = chosen_view // view_dev
    owner_hits = (owner_of[:, None] == jnp.arange(owners, dtype=jnp.int32)[None, :]).astype(
        jnp.int32
    )
    earlier = jnp.cumsum(owner_hits, axis=0) - owner_hits
    slot_rank = jnp.sum(earlier * owner_hits, axis=1)
    target = owner_of * capacity + slot_rank
    matches = target[None, :] == jnp.arange(buffer_len, dtype=jnp.int32)[:, None]
    source = jnp.sum(
        jnp.where(matches, jnp.arange(slot_count, dtype=jnp.int32)[None, :], 0), axis=1
    )
    filled = jnp.any(matches, axis=1)
    patch_rows = jnp.where(filled[:, None, None], patches[0][source], jnp.zeros((), jnp.bfloat16))
    slot_meta = jnp.stack(
        [
            slot_tilt[0].astype(jnp.float32),
            (chosen_view % view_dev).astype(jnp.float32),
            defocus[0].astype(jnp.float32),
            slot_pos[0, 0].astype(jnp.float32),
            slot_pos[1, 0].astype(jnp.float32),
            jnp.ones((slot_count,), jnp.float32),
        ],
        axis=1,
    )
    meta_rows = jnp.where(filled[:, None], slot_meta[source], 0.0).astype(jnp.bfloat16)
    patch_buffer = patch_rows.reshape(owners, capacity, pixels, pixels)
    meta_buffer = meta_rows.reshape(owners, capacity, 6)
    row_span = projections.shape[3]
    freq_rows = lax.axis_index("rep") * row_span + jnp.arange(row_span, dtype=jnp.int32)
    row_table, col_table = dft_tables(freq_rows, pixels)
    row_total = freq_rows.shape[0]
    projected_flat = projections.reshape(view_dev * tilt_dev, 2, row_total, pixels)
    tilt_iota = jnp.arange(tilt_dev, dtype=jnp.int32)
    view_iota = jnp.arange(view_dev, dtype=jnp.int32)

    def one_block(inputs):
        patch_blk, index_blk, focus_blk, shift_blk = inputs
        ref_blk = projected_flat[index_blk]
        first_pass = jnp.einsum(
            "fy,byx->bfx", row_table, patch_blk, preferred_element_type=jnp.float32
        ).astype(jnp.bfloat16)
        spectrum = jnp.einsum(
            "bfx,xk->bfk", first_pass, col_table, preferred_element_type=jnp.float32
        )
        return spectral_terms(spectrum, ref_blk, focus_blk, shift_blk, freq_rows, pixels)

    patch_in = lax.all_to_all(patch_buffer, "dom", split_axis=0, concat_axis=0, tiled=True)
    meta_in = lax.all_to_all(meta_buffer, "dom", split_axis=0, concat_axis=0, tiled=True)
    senders = patch_in.shape[0]
    per_sender = patch_in.shape[1]
    slot_total = senders * per_sender
    meta_flat = meta_in.reshape(slot_total, 6).astype(jnp.float32)
    tilt_match = meta_flat[:, 0:1] == tilt_iota.astype(jnp.float32)[None, :]
    view_match = meta_flat[:, 1:2] == view_iota.astype(jnp.float32)[None, :]
    tilt_local = jnp.sum(jnp.where(tilt_match, tilt_iota[None, :], 0), axis=1)
    view_local = jnp.sum(jnp.where(view_match, view_iota[None, :], 0), axis=1)
    weights = node_weights(meta_flat[:, 3], meta_flat[:, 4], GRID)
    shifts = jnp.sum(warp_grid[tilt_local] * weights[:, None, :], axis=2)
    block_len = math.gcd(slot_total, 16)
    block_count = slot_total // block_len
    per_slot = lax.map(
        one_block,
        (
            patch_in.reshape(block_count, block_len, pixels, pixels),
            (view_local * tilt_dev + tilt_local).reshape(block_count, block_len),
            meta_flat[:, 2].reshape(block_count, block_len),
            shifts.reshape(block_count, block_len, 2),
        ),
    ).reshape(slot_total, 3)
    node_coef = (
        tilt_match.astype(jnp.float32)[:, :, None]
        * per_slot[:, None, 1:3]
        * meta_flat[:, 5, None, None]
    ).reshape(senders, per_sender, 2 * tilt_dev)
    returned = lax.all_to_all(
        per_slot.reshape(senders, per_sender, 3), "dom", split_axis=0, concat_axis=0, tiled=True
    )
    weight_all = weights.reshape(senders, per_sender, node_count)
    own_terms = returned.reshape(buffer_len, 3)[target]
    summed = lax.psum(own_terms, "rep")
    slot_terms = summed.T[:, None, :]
    gradient = jnp.dot(
        node_coef.reshape(-1, 2 * tilt_dev).T,
        weight_all.reshape(-1, node_count),
        precision=lax.Precision.HIGHEST,
        preferred_element_type=jnp.float32,
    ).reshape(tilt_dev, 2, node_count)
    whole_grad = lax.psum(gradient, ("dom", "rep"))
    new_warp = warp_grid - whole_grad / jnp.sqrt(
        whole_grad * whole_grad + TRUST_FLOOR * TRUST_FLOOR
    )
    return (slot_terms, new_warp)


CORES = 2
EXTRA_ROWS = 8
RANK = 16
DELTA = math.asin(AMPLITUDE)
F32 = jnp.float32
BF16 = jnp.bfloat16


def two_parts(values):
    high = values.astype(BF16)
    return high, (values - high.astype(F32)).astype(BF16)


def fold_references(projections, pixels):
    half = pixels // 2
    refs = projections.reshape(-1, 2, pixels, pixels)
    k = jnp.arange(pixels, dtype=jnp.int32)
    lane_freq = k % half
    lane_part = k // half
    chan = jnp.arange(2, dtype=jnp.int32)
    same_part = chan[:, None, None] == lane_part[None, None, :]
    pick = (same_part & (k[None, :, None] == lane_freq[None, None, :])).astype(BF16)
    flip = (
        same_part
        & (k[None, :, None] == pixels - lane_freq[None, None, :])
        & (lane_freq > 0)[None, None, :]
    ).astype(BF16)
    rows_flip = ((k[:, None] + k[None, :]) % pixels == 0) & (k != half)[:, None]
    straight = jnp.einsum("ncyx,cxl->nyl", refs, pick, preferred_element_type=F32)
    mirrored = jnp.einsum("ncyx,cxl->nyl", refs, flip, preferred_element_type=F32).astype(BF16)
    turned = jnp.einsum("zy,nyl->nzl", rows_flip.astype(BF16), mirrored, preferred_element_type=F32)
    sign = jnp.where(lane_part == 0, 1.0, -1.0)
    packed = (straight + sign * turned).astype(BF16)
    column = refs[:, :, :, half]
    right = mirrored[:, half : half + 1, :]
    table = jnp.arange(2 * pixels, dtype=jnp.int32)
    focus = jnp.where(
        table < pixels, 1.0 + table / pixels, 2.0 + (table - pixels) / (pixels // 2)
    ).astype(F32)
    freq = signed_freq(k, pixels)
    chi = math.pi * focus[None, :] * (freq * freq / (half * half))[:, None]
    real = refs[:, 0].astype(F32)
    imag = refs[:, 1].astype(F32)
    power = real * real + imag * imag
    waves = jnp.concatenate([jnp.cos(2.0 * chi), jnp.sin(2.0 * chi)], axis=1).astype(BF16)
    mixed = jnp.einsum("nyx,xd->nyd", power.astype(BF16), waves, preferred_element_type=F32)
    turn = 2.0 * chi + 2.0 * DELTA
    weights = jnp.concatenate([jnp.cos(turn), -jnp.sin(turn)], axis=1)
    swing = jnp.sum(mixed * weights[None], axis=1)
    swing = swing[:, : 2 * pixels] + swing[:, 2 * pixels :]
    total = 0.5 * jnp.sum(power, axis=(1, 2))[:, None] - 0.5 * swing
    high, low = two_parts(total)
    count = refs.shape[0]
    extra = jnp.concatenate(
        [
            column,
            right,
            high.reshape(count, 2, pixels),
            low.reshape(count, 2, pixels),
            jnp.zeros((count, EXTRA_ROWS - 7, pixels), BF16),
        ],
        axis=1,
    )
    return jnp.concatenate([packed, extra], axis=1)


def line_gather_kernel(chips, own_ref, all_ref, right_send, right_recv, left_send, left_recv,
                       pair_send, pair_recv, local_sem):
    me = lax.axis_index("dom")
    chip = me // CORES
    core = me % CORES
    partner = chip * CORES + (1 - core)
    right = me + CORES
    left = me - CORES
    last = chips - 1
    barrier = pltpu.get_barrier_semaphore()

    def greet(device):
        pl.semaphore_signal(
            barrier, inc=1, device_id={"dom": device}, device_id_type=pl.DeviceIdType.MESH
        )

    greet(partner)

    @pl.when(chip < last)
    def _():
        greet(right)

    @pl.when(chip > 0)
    def _():
        greet(left)

    inner = (chip > 0) & (chip < last)

    @pl.when(inner)
    def _():
        pl.semaphore_wait(barrier, 3)

    @pl.when(jnp.logical_not(inner))
    def _():
        pl.semaphore_wait(barrier, 2)

    def copy(src, owner, send, recv, target):
        return pltpu.make_async_remote_copy(
            src_ref=src, dst_ref=all_ref.at[owner], send_sem=send, recv_sem=recv,
            device_id={"dom": target}, device_id_type=pl.DeviceIdType.MESH,
        )

    def to_right(src, hop):
        return copy(src, me - CORES * hop, right_send.at[hop], right_recv.at[hop], right)

    def to_left(src, hop):
        return copy(src, me + CORES * hop, left_send.at[hop], left_recv.at[hop], left)

    def to_pair(src, owner):
        slot = owner // CORES
        return copy(src, owner, pair_send.at[slot], pair_recv.at[slot], partner)

    keep = pltpu.make_async_copy(own_ref, all_ref.at[me], local_sem)

    @pl.when(chip < last)
    def _():
        to_right(own_ref, 0).start()

    @pl.when(chip > 0)
    def _():
        to_left(own_ref, 0).start()

    to_pair(own_ref, me).start()
    keep.start()
    for hop in range(1, chips):
        @pl.when(chip >= hop)
        def _():
            owner = me - CORES * hop
            block = all_ref.at[owner]
            copy(block, owner, right_send.at[hop - 1], right_recv.at[hop - 1], right).wait_recv()

            @pl.when(chip < last)
            def _():
                to_right(block, hop).start()

            to_pair(block, owner).start()

        @pl.when(chip + hop <= last)
        def _():
            owner = me + CORES * hop
            block = all_ref.at[owner]
            copy(block, owner, left_send.at[hop - 1], left_recv.at[hop - 1], left).wait_recv()

            @pl.when(chip > 0)
            def _():
                to_left(block, hop).start()

            to_pair(block, owner).start()

    for hop in range(chips):
        @pl.when((chip >= hop) & (chip < last))
        def _():
            to_right(own_ref, hop).wait_send()

        @pl.when((chip + hop <= last) & (chip > 0))
        def _():
            to_left(own_ref, hop).wait_send()

    for other in range(chips):
        owner = other * CORES + core
        to_pair(own_ref, owner).wait_send()
        incoming = other * CORES + (1 - core)
        copy(own_ref, incoming, pair_send.at[other], pair_recv.at[other], partner).wait_recv()
    keep.wait()


def line_gather(block):
    owners = lax.axis_size("dom")
    chips = owners // CORES
    dma = pltpu.SemaphoreType.DMA((chips,))
    return pl.pallas_call(
        functools.partial(line_gather_kernel, chips),
        out_shape=jax.ShapeDtypeStruct((owners,) + block.shape, block.dtype),
        in_specs=[pl.BlockSpec(memory_space=pl.ANY)],
        out_specs=pl.BlockSpec(memory_space=pl.ANY),
        scratch_shapes=[dma] * 6 + [pltpu.SemaphoreType.DMA],
        compiler_params=pltpu.CompilerParams(collective_id=0, has_side_effects=True),
        name="line_gather",
    )(block)


def slot_kernel(which_ref, patch_ref, refs_ref, cols_ref, rows_ref, first_ref, second_ref, nyq_ref,
                sums_ref, extra_ref):
    slots, pixels = patch_ref.shape[0], patch_ref.shape[1]
    half = pixels // 2
    row_index = lax.broadcasted_iota(jnp.int32, (pixels, pixels), 0)
    freq_y = jnp.where(row_index < half, row_index, row_index - pixels).astype(F32)

    def pair(step, carry):
        base = step * 2
        both = jnp.concatenate([patch_ref[base], patch_ref[base + 1]], axis=1)
        first = jnp.dot(first_ref[...], both, preferred_element_type=F32).astype(BF16)
        for part in range(2):
            slot = base + part
            which = which_ref[slot]
            mine = first[:, part * pixels : (part + 1) * pixels]
            wide = jnp.concatenate([mine[:pixels], mine[pixels:]], axis=1)
            spectrum = jnp.dot(wide, second_ref[...], preferred_element_type=F32)
            line = lax.dot_general(
                nyq_ref[...], mine, (((1,), (1,)), ((), ())), preferred_element_type=F32
            )
            turn = jnp.dot(cols_ref[slot], rows_ref[slot], preferred_element_type=F32)
            ref = refs_ref[which, :pixels].astype(F32)
            plain = spectrum[:, :pixels]
            along = plain * ref
            across = spectrum[:, pixels:] * ref
            cosine = turn[:, :pixels]
            sine = turn[:, pixels:]
            real = cosine * along - sine * across
            imag = sine * along + cosine * across
            sums_ref[slot, 0:1] = jnp.sum(real, axis=0, keepdims=True)
            sums_ref[slot, 1:2] = jnp.sum(imag, axis=0, keepdims=True)
            sums_ref[slot, 2:3] = jnp.sum(imag * freq_y, axis=0, keepdims=True)
            sums_ref[slot, 3:4] = jnp.sum(plain * plain, axis=0, keepdims=True)
            sums_ref[slot, 4:5] = plain[half : half + 1]
            sums_ref[slot, 5:6] = line[0:1, :pixels]
            sums_ref[slot, 6:7] = line[0:1, pixels:]
            sums_ref[slot, 7:8] = jnp.zeros((1, pixels), F32)
            extra_ref[slot] = refs_ref[which, pixels:].astype(F32)
        return carry

    lax.fori_loop(0, slots // 2, pair, 0)


def slot_sums(which, patches, refs, cols, rows, first, second, nyquist):
    slots, pixels = patches.shape[0], patches.shape[1]
    vmem = pl.BlockSpec(memory_space=pltpu.VMEM)
    return pl.pallas_call(
        slot_kernel,
        out_shape=(
            jax.ShapeDtypeStruct((slots, 8, pixels), F32),
            jax.ShapeDtypeStruct((slots, EXTRA_ROWS, pixels), F32),
        ),
        in_specs=[pl.BlockSpec(memory_space=pltpu.SMEM)] + [vmem] * 7,
        out_specs=(vmem, vmem),
        compiler_params=pltpu.CompilerParams(vmem_limit_bytes=48 * 1024 * 1024),
        name="slot_sums",
    )(which, patches, refs, cols, rows, first, second, nyquist)


def pass_tables(pixels):
    half = pixels // 2
    row_table, col_table = dft_tables(jnp.arange(pixels, dtype=jnp.int32), pixels)
    cosine = col_table[:, :half]
    sine = col_table[:, pixels : pixels + half]
    real = jnp.concatenate([cosine, -sine], axis=0)
    imag = jnp.concatenate([-sine, -cosine], axis=0)
    second = jnp.concatenate([real, imag, imag, -real], axis=1)
    nyquist = jnp.broadcast_to(col_table[:, half][None, :], (16, pixels))
    return row_table, second, nyquist


def slot_factors(focus, shifts, pixels):
    half = pixels // 2
    freq_y = signed_freq(jnp.arange(pixels, dtype=jnp.int32), pixels)
    freq_x = jnp.arange(half, dtype=jnp.int32).astype(F32)
    chi_y = math.pi * focus[:, None] * (freq_y * freq_y / (half * half))[None, :] + DELTA
    chi_x = math.pi * focus[:, None] * (freq_x * freq_x / (half * half))[None, :]
    step = 2.0 * math.pi / pixels
    phi_y = step * shifts[:, 1:2] * freq_y[None, :]
    phi_x = step * shifts[:, 0:1] * freq_x[None, :]
    s_y, c_y, p_y, q_y = jnp.sin(chi_y), jnp.cos(chi_y), jnp.cos(phi_y), jnp.sin(phi_y)
    c_x, s_x, p_x, q_x = jnp.cos(chi_x), jnp.sin(chi_x), jnp.cos(phi_x), jnp.sin(phi_x)
    cols = jnp.stack([s_y * p_y, s_y * q_y, c_y * p_y, c_y * q_y], axis=2)
    a, b, c, d = c_x * p_x, c_x * q_x, s_x * p_x, s_x * q_x
    for_cos = jnp.stack([-a, b, -c, d], axis=1)
    for_sin = jnp.stack([-b, -a, -d, -c], axis=1)
    rows = jnp.concatenate([for_cos, for_cos, for_sin, for_sin], axis=2)
    col_high, col_low = two_parts(cols)
    row_high, row_low = two_parts(rows)
    cols = jnp.concatenate([col_high, col_high, col_low, jnp.zeros_like(col_low)], axis=2)
    rows = jnp.concatenate([row_high, row_low, row_high, jnp.zeros_like(row_low)], axis=1)
    return cols, rows


def line_terms(spec_re, spec_im, ref_re, ref_im, chi, phi):
    contrast = -jnp.sin(chi + DELTA)
    cosine = jnp.cos(phi)
    sine = jnp.sin(phi)
    model_re = contrast * (ref_re * cosine + ref_im * sine)
    model_im = contrast * (ref_im * cosine - ref_re * sine)
    return spec_re * model_re + spec_im * model_im, spec_im * model_re - spec_re * model_im


def finish_terms(sums, extra, focus, shifts, pixels):
    half = pixels // 2
    k = jnp.arange(pixels, dtype=jnp.int32)
    freq = signed_freq(k, pixels)
    lane_freq = (k % half).astype(F32)
    step = 2.0 * math.pi / pixels
    norm = 1.0 / (half * half)
    match = jnp.sum(sums[:, 0], axis=1)
    grad_x = jnp.sum(sums[:, 1] * lane_freq, axis=1)
    grad_y = jnp.sum(sums[:, 2], axis=1)
    power = jnp.sum(sums[:, 3] * jnp.where(lane_freq > 0, 2.0, 1.0), axis=1)
    d = focus[:, None]
    s_x, s_y = shifts[:, 0:1], shifts[:, 1:2]
    col_re, col_im = sums[:, 5], -sums[:, 6]
    power = power + jnp.sum(col_re * col_re + col_im * col_im, axis=1)
    along, across = line_terms(
        col_re, col_im, extra[:, 0], extra[:, 1],
        math.pi * d * (freq * freq * norm + 1.0), step * (freq * s_y - half * s_x),
    )
    match = match + jnp.sum(along, axis=1)
    grad_x = grad_x - half * jnp.sum(across, axis=1)
    grad_y = grad_y + jnp.sum(across * freq, axis=1)
    f = lane_freq[:half]
    along, across = line_terms(
        sums[:, 4, :half], -sums[:, 4, half:], extra[:, 2, :half], extra[:, 2, half:],
        math.pi * d * (f * f * norm + 1.0), step * (-f * s_x - half * s_y),
    )
    match = match + jnp.sum(along, axis=1)
    grad_x = grad_x - jnp.sum(across * f, axis=1)
    grad_y = grad_y - half * jnp.sum(across, axis=1)
    place = jnp.where(
        focus < 2.0, (focus - 1.0) * pixels, pixels + (focus - 2.0) * half
    )
    table_high = extra[:, 3:5].reshape(-1, 2 * pixels)
    table_low = extra[:, 5:7].reshape(-1, 2 * pixels)
    hit = place[:, None] == jnp.arange(2 * pixels, dtype=jnp.int32).astype(F32)[None, :]
    model_power = jnp.sum(jnp.where(hit, table_high + table_low, 0.0), axis=1)
    area = 1.0 / (pixels * pixels)
    energy = (power + model_power - 2.0 * match) * area
    return jnp.stack([energy, 2.0 * area * step * grad_x, 2.0 * area * step * grad_y], axis=0)


def on_device_gathered(
    patches, slot_view, slot_tilt, slot_pos, defocus, projections, warp_grid
):
    pixels = patches.shape[-1]
    tilt_dev = warp_grid.shape[0]
    node_count = warp_grid.shape[2]
    tilt = slot_tilt[0]
    refs = line_gather(fold_references(projections, pixels))
    refs = refs.reshape(-1, pixels + EXTRA_ROWS, pixels)
    weights = node_weights(slot_pos[0, 0].astype(F32), slot_pos[1, 0].astype(F32), GRID)
    tilt_match = (tilt[:, None] == jnp.arange(tilt_dev, dtype=jnp.int32)[None, :]).astype(F32)
    chosen = jnp.dot(
        tilt_match, warp_grid.reshape(tilt_dev, -1), precision=lax.Precision.HIGHEST
    ).reshape(-1, 2, node_count)
    shifts = jnp.sum(chosen * weights[:, None, :], axis=2)
    focus = defocus[0].astype(F32)
    cols, rows = slot_factors(focus, shifts, pixels)
    first, second, nyquist = pass_tables(pixels)
    which = slot_view[0, :, 0] * tilt_dev + tilt
    sums, extra = slot_sums(which, patches[0], refs, cols, rows, first, second, nyquist)
    terms = finish_terms(sums, extra, focus, shifts, pixels)
    coef = (tilt_match.T[:, None, :] * terms[None, 1:3, :]).reshape(2 * tilt_dev, -1)
    gradient = jnp.dot(
        coef, weights, precision=lax.Precision.HIGHEST, preferred_element_type=F32
    ).reshape(tilt_dev, 2, node_count)
    whole_grad = lax.psum(gradient, "dom")
    new_warp = warp_grid - whole_grad / jnp.sqrt(
        whole_grad * whole_grad + TRUST_FLOOR * TRUST_FLOOR
    )
    return (terms[:, None, :], new_warp)


def solution(mesh):
    body = on_device if mesh.shape["rep"] > 1 else on_device_gathered
    in_specs = (
        P(("groups", "tilt"), "dom", None, None),
        P(("groups", "tilt"), "dom", None),
        P(("groups", "tilt"), "dom"),
        P(None, ("groups", "tilt"), "dom"),
        P(("groups", "tilt"), "dom"),
        P(("groups", "dom"), "tilt", None, "rep", None),
        P(("groups", "tilt"), None, None),
    )
    out_specs = (P(None, ("groups", "tilt"), "dom"), P(("groups", "tilt"), None, None))
    return jax.shard_map(
        body, mesh=mesh, in_specs=in_specs, out_specs=out_specs, check_vma=False
    )
```

```python
import functools
import math

import jax
import jax.numpy as jnp
from jax import lax
from jax.experimental import pallas as pl
from jax.experimental.pallas import tpu as pltpu
from jax.sharding import PartitionSpec as P

GRID = 16


AMPLITUDE = 0.07
TRUST_FLOOR = 0.02


def signed_freq(index, pixels):
    return jnp.where(index < pixels // 2, index, index - pixels).astype(jnp.float32)


def dft_tables(freq_rows, pixels):
    columns = jnp.arange(pixels, dtype=jnp.int32)
    table_scale = 1.0 / math.sqrt(pixels)
    turns_rows = (freq_rows[:, None] * columns[None, :] % pixels).astype(jnp.float32) * (
        2.0 * math.pi / pixels
    )
    turns_full = (columns[:, None] * columns[None, :] % pixels).astype(jnp.float32) * (
        2.0 * math.pi / pixels
    )
    row_table = jnp.concatenate([jnp.cos(turns_rows), jnp.sin(turns_rows)], axis=0) * table_scale
    col_table = jnp.concatenate([jnp.cos(turns_full), jnp.sin(turns_full)], axis=1) * table_scale
    return (row_table.astype(jnp.bfloat16), col_table.astype(jnp.bfloat16))


def node_weights(pos_x, pos_y, grid_side):
    knot_pos = jnp.arange(grid_side, dtype=jnp.int32).astype(jnp.float32)
    weight_x = jnp.maximum(0.0, 1.0 - jnp.abs(pos_x[:, None] * (grid_side - 1) - knot_pos[None, :]))
    weight_y = jnp.maximum(0.0, 1.0 - jnp.abs(pos_y[:, None] * (grid_side - 1) - knot_pos[None, :]))
    return (weight_y[:, :, None] * weight_x[:, None, :]).reshape(
        pos_x.shape[0], grid_side * grid_side
    )


def spectral_terms(spectrum, ref_blk, focus_blk, shift_blk, freq_rows, pixels):
    row_total = freq_rows.shape[0]
    v_one_cos = spectrum[:, :row_total, :pixels]
    v_one_sin = spectrum[:, :row_total, pixels:]
    v_two_cos = spectrum[:, row_total:, :pixels]
    v_two_sin = spectrum[:, row_total:, pixels:]
    real_part = v_one_cos - v_two_sin
    imag_part = -(v_one_sin + v_two_cos)
    freq_y = signed_freq(freq_rows, pixels)[None, :, None]
    freq_x = signed_freq(jnp.arange(pixels, dtype=jnp.int32), pixels)[None, None, :]
    nyquist = pixels / 2.0
    radius = (freq_y * freq_y + freq_x * freq_x) / (nyquist * nyquist)
    aberration = math.pi * focus_blk[:, None, None] * radius
    contrast = -(
        math.sqrt(1.0 - AMPLITUDE * AMPLITUDE) * jnp.sin(aberration)
        + AMPLITUDE * jnp.cos(aberration)
    )
    phase_angle = (
        2.0
        * math.pi
        / pixels
        * (freq_x * shift_blk[:, 0, None, None] + freq_y * shift_blk[:, 1, None, None])
    )
    cosine = jnp.cos(phase_angle)
    sine_part = jnp.sin(phase_angle)
    ref_real = ref_blk[:, 0].astype(jnp.float32)
    ref_imag = ref_blk[:, 1].astype(jnp.float32)
    model_real = contrast * (ref_real * cosine + ref_imag * sine_part)
    model_imag = contrast * (ref_imag * cosine - ref_real * sine_part)
    diff_real = real_part - model_real
    diff_imag = imag_part - model_imag
    inverse_area = 1.0 / (pixels * pixels)
    energy = jnp.sum(diff_real * diff_real + diff_imag * diff_imag, axis=(1, 2)) * inverse_area
    cross_term = diff_imag * model_real - diff_real * model_imag
    grad_x = 2.0 * inverse_area * jnp.sum(2.0 * math.pi / pixels * freq_x * cross_term, axis=(1, 2))
    grad_y = 2.0 * inverse_area * jnp.sum(2.0 * math.pi / pixels * freq_y * cross_term, axis=(1, 2))
    return jnp.stack([energy, grad_x, grad_y], axis=1)


def on_device(patches, slot_view, slot_tilt, slot_pos, defocus, projections, warp_grid):
    owners = lax.axis_size("dom")
    slot_count = patches.shape[1]
    pixels = patches.shape[-1]
    view_dev = projections.shape[0]
    tilt_dev = warp_grid.shape[0]
    node_count = warp_grid.shape[2]
    capacity = 3 * slot_count // (2 * owners)
    buffer_len = owners * capacity
    chosen_view = slot_view[0, :, 0]
    owner_of = chosen_view // view_dev
    owner_hits = (owner_of[:, None] == jnp.arange(owners, dtype=jnp.int32)[None, :]).astype(
        jnp.int32
    )
    earlier = jnp.cumsum(owner_hits, axis=0) - owner_hits
    slot_rank = jnp.sum(earlier * owner_hits, axis=1)
    target = owner_of * capacity + slot_rank
    matches = target[None, :] == jnp.arange(buffer_len, dtype=jnp.int32)[:, None]
    source = jnp.sum(
        jnp.where(matches, jnp.arange(slot_count, dtype=jnp.int32)[None, :], 0), axis=1
    )
    filled = jnp.any(matches, axis=1)
    patch_rows = jnp.where(filled[:, None, None], patches[0][source], jnp.zeros((), jnp.bfloat16))
    slot_meta = jnp.stack(
        [
            slot_tilt[0].astype(jnp.float32),
            (chosen_view % view_dev).astype(jnp.float32),
            defocus[0].astype(jnp.float32),
            slot_pos[0, 0].astype(jnp.float32),
            slot_pos[1, 0].astype(jnp.float32),
            jnp.ones((slot_count,), jnp.float32),
        ],
        axis=1,
    )
    meta_rows = jnp.where(filled[:, None], slot_meta[source], 0.0).astype(jnp.bfloat16)
    patch_buffer = patch_rows.reshape(owners, capacity, pixels, pixels)
    meta_buffer = meta_rows.reshape(owners, capacity, 6)
    row_span = projections.shape[3]
    freq_rows = lax.axis_index("rep") * row_span + jnp.arange(row_span, dtype=jnp.int32)
    row_table, col_table = dft_tables(freq_rows, pixels)
    row_total = freq_rows.shape[0]
    projected_flat = projections.reshape(view_dev * tilt_dev, 2, row_total, pixels)
    tilt_iota = jnp.arange(tilt_dev, dtype=jnp.int32)
    view_iota = jnp.arange(view_dev, dtype=jnp.int32)

    def one_block(inputs):
        patch_blk, index_blk, focus_blk, shift_blk = inputs
        ref_blk = projected_flat[index_blk]
        first_pass = jnp.einsum(
            "fy,byx->bfx", row_table, patch_blk, preferred_element_type=jnp.float32
        ).astype(jnp.bfloat16)
        spectrum = jnp.einsum(
            "bfx,xk->bfk", first_pass, col_table, preferred_element_type=jnp.float32
        )
        return spectral_terms(spectrum, ref_blk, focus_blk, shift_blk, freq_rows, pixels)

    patch_in = lax.all_to_all(patch_buffer, "dom", split_axis=0, concat_axis=0, tiled=True)
    meta_in = lax.all_to_all(meta_buffer, "dom", split_axis=0, concat_axis=0, tiled=True)
    senders = patch_in.shape[0]
    per_sender = patch_in.shape[1]
    slot_total = senders * per_sender
    meta_flat = meta_in.reshape(slot_total, 6).astype(jnp.float32)
    tilt_match = meta_flat[:, 0:1] == tilt_iota.astype(jnp.float32)[None, :]
    view_match = meta_flat[:, 1:2] == view_iota.astype(jnp.float32)[None, :]
    tilt_local = jnp.sum(jnp.where(tilt_match, tilt_iota[None, :], 0), axis=1)
    view_local = jnp.sum(jnp.where(view_match, view_iota[None, :], 0), axis=1)
    weights = node_weights(meta_flat[:, 3], meta_flat[:, 4], GRID)
    shifts = jnp.sum(warp_grid[tilt_local] * weights[:, None, :], axis=2)
    block_len = math.gcd(slot_total, 16)
    block_count = slot_total // block_len
    per_slot = lax.map(
        one_block,
        (
            patch_in.reshape(block_count, block_len, pixels, pixels),
            (view_local * tilt_dev + tilt_local).reshape(block_count, block_len),
            meta_flat[:, 2].reshape(block_count, block_len),
            shifts.reshape(block_count, block_len, 2),
        ),
    ).reshape(slot_total, 3)
    node_coef = (
        tilt_match.astype(jnp.float32)[:, :, None]
        * per_slot[:, None, 1:3]
        * meta_flat[:, 5, None, None]
    ).reshape(senders, per_sender, 2 * tilt_dev)
    returned = lax.all_to_all(
        per_slot.reshape(senders, per_sender, 3), "dom", split_axis=0, concat_axis=0, tiled=True
    )
    weight_all = weights.reshape(senders, per_sender, node_count)
    own_terms = returned.reshape(buffer_len, 3)[target]
    summed = lax.psum(own_terms, "rep")
    slot_terms = summed.T[:, None, :]
    gradient = jnp.dot(
        node_coef.reshape(-1, 2 * tilt_dev).T,
        weight_all.reshape(-1, node_count),
        precision=lax.Precision.HIGHEST,
        preferred_element_type=jnp.float32,
    ).reshape(tilt_dev, 2, node_count)
    whole_grad = lax.psum(gradient, ("dom", "rep"))
    new_warp = warp_grid - whole_grad / jnp.sqrt(
        whole_grad * whole_grad + TRUST_FLOOR * TRUST_FLOOR
    )
    return (slot_terms, new_warp)


CORES = 2
EXTRA_ROWS = 8
DELTA = math.asin(AMPLITUDE)
F32 = jnp.float32
BF16 = jnp.bfloat16


def fold_kernel(refs_ref, pick_ref, turn_ref, unit_ref, waves_ref, weights_ref, out_ref):
    pixels = turn_ref.shape[0]
    half = pixels // 2
    lane = lax.broadcasted_iota(jnp.int32, (1, pixels), 1)
    sign = jnp.where(lane < half, 1.0, -1.0)

    def one(n, carry):
        real, imag = refs_ref[n, 0], refs_ref[n, 1]
        wide = jnp.concatenate([real, imag], axis=1)
        picked = jnp.dot(wide, pick_ref[...], preferred_element_type=F32)
        mirrored = picked[:, pixels:]
        turned = jnp.dot(turn_ref[...], mirrored.astype(BF16), preferred_element_type=F32)
        out_ref[n, :pixels] = (picked[:, :pixels] + sign * turned).astype(BF16)
        tall = jnp.concatenate([real, imag], axis=0)
        column = lax.dot_general(
            unit_ref[...], tall, (((1,), (1,)), ((), ())), preferred_element_type=F32
        )
        r, i = real.astype(F32), imag.astype(F32)
        power = r * r + i * i
        mixed = jnp.dot(power.astype(BF16), waves_ref[...], preferred_element_type=F32)
        swing = jnp.sum(mixed * weights_ref[...], axis=0, keepdims=True)
        swing = swing[:, : 2 * pixels] + swing[:, 2 * pixels :]
        total = 0.5 * jnp.sum(power) - 0.5 * swing
        high = total.astype(BF16).astype(F32)
        low = total - high
        extra = jnp.concatenate(
            [
                column[0:1, :pixels],
                column[0:1, pixels:],
                mirrored[half : half + 1],
                high[:, :pixels],
                high[:, pixels:],
                low[:, :pixels],
                low[:, pixels:],
                jnp.zeros((EXTRA_ROWS - 7, pixels), F32),
            ],
            axis=0,
        )
        out_ref[n, pixels:] = extra.astype(BF16)
        return carry

    lax.fori_loop(0, refs_ref.shape[0], one, 0)


def fold_references(projections, pixels):
    half = pixels // 2
    refs = projections.reshape(-1, 2, pixels, pixels)
    count = refs.shape[0]
    k = jnp.arange(pixels, dtype=jnp.int32)
    lane_freq = k % half
    lane_part = k // half
    chan = jnp.arange(2, dtype=jnp.int32)
    same_part = chan[:, None, None] == lane_part[None, None, :]
    pick = same_part & (k[None, :, None] == lane_freq[None, None, :])
    flip = (
        same_part
        & (k[None, :, None] == pixels - lane_freq[None, None, :])
        & (lane_freq > 0)[None, None, :]
    )
    picks = jnp.concatenate([pick, flip], axis=2).reshape(2 * pixels, 2 * pixels).astype(BF16)
    turn = (((k[:, None] + k[None, :]) % pixels == 0) & (k != half)[:, None]).astype(BF16)
    unit = jnp.broadcast_to((k == half).astype(BF16)[None, :], (16, pixels))
    table = jnp.arange(2 * pixels, dtype=jnp.int32)
    focus = jnp.where(
        table < pixels, 1.0 + table / pixels, 2.0 + (table - pixels) / (pixels // 2)
    ).astype(F32)
    freq = signed_freq(k, pixels)
    chi = math.pi * focus[None, :] * (freq * freq / (half * half))[:, None]
    chi = jnp.concatenate([chi, chi + 0.25 * math.pi], axis=1) * 2.0
    waves = jnp.cos(jnp.concatenate([chi[:, : 2 * pixels], chi[:, 2 * pixels :] - math.pi], axis=1))
    weights = jnp.cos(chi + 2.0 * DELTA)
    rows = pixels + EXTRA_ROWS
    group = math.gcd(count, 5)
    full = lambda x: pl.BlockSpec(x.shape, lambda i: (0, 0))
    tables = (picks, turn, unit, waves.astype(BF16), weights)
    return pl.pallas_call(
        fold_kernel,
        grid=(count // group,),
        out_shape=jax.ShapeDtypeStruct((count, rows, pixels), BF16),
        in_specs=[pl.BlockSpec((group, 2, pixels, pixels), lambda i: (i, 0, 0, 0))]
        + [full(x) for x in tables],
        out_specs=pl.BlockSpec((group, rows, pixels), lambda i: (i, 0, 0)),
        name="fold_references",
    )(refs, *tables)


def gather_kernel(chips, cap, src_ref, which_ref, own_ref, patch_ref, meta_ref, first_ref,
                  second_ref, nyq_ref, sums_ref, extra_ref, factor_ref, *rest):
    lefts, rights = rest[: chips - 1], rest[chips - 1 : 2 * chips - 2]
    left_pairs, right_pairs = rest[2 * chips - 2 : 3 * chips - 3], rest[3 * chips - 3 : 4 * chips - 4]
    (pair_ref, rs, rr, ls, lr, lps, lpr, rps, rpr, ps, pr) = rest[4 * chips - 4 :]
    pixels = patch_ref.shape[1]
    half = pixels // 2
    me = lax.axis_index("dom")
    chip = me // CORES
    core = me % CORES
    partner = chip * CORES + (1 - core)
    right = me + CORES
    left = me - CORES
    last = chips - 1
    barrier = pltpu.get_barrier_semaphore()

    def greet(device):
        pl.semaphore_signal(
            barrier, inc=1, device_id={"dom": device}, device_id_type=pl.DeviceIdType.MESH
        )

    greet(partner)

    @pl.when(chip < last)
    def _():
        greet(right)

    @pl.when(chip > 0)
    def _():
        greet(left)

    inner = (chip > 0) & (chip < last)

    @pl.when(inner)
    def _():
        pl.semaphore_wait(barrier, 3)

    @pl.when(jnp.logical_not(inner))
    def _():
        pl.semaphore_wait(barrier, 2)

    def copy(src, dst, send, recv, target):
        return pltpu.make_async_remote_copy(
            src_ref=src, dst_ref=dst, send_sem=send, recv_sem=recv,
            device_id={"dom": target}, device_id_type=pl.DeviceIdType.MESH,
        )

    def to_right(hop):
        src = own_ref if hop == 0 else lefts[hop - 1]
        return copy(src, lefts[hop], rs.at[hop], rr.at[hop], right)

    def to_left(hop):
        src = own_ref if hop == 0 else rights[hop - 1]
        return copy(src, rights[hop], ls.at[hop], lr.at[hop], left)

    def pair_left(hop):
        return copy(lefts[hop], left_pairs[hop], lps.at[hop], lpr.at[hop], partner)

    def pair_right(hop):
        return copy(rights[hop], right_pairs[hop], rps.at[hop], rpr.at[hop], partner)

    pair_own = copy(own_ref, pair_ref, ps, pr, partner)

    @pl.when(chip < last)
    def _():
        to_right(0).start()

    @pl.when(chip > 0)
    def _():
        to_left(0).start()

    pair_own.start()

    row_index = lax.broadcasted_iota(jnp.int32, (pixels, pixels), 0)
    freq_y = jnp.where(row_index < half, row_index, row_index - pixels).astype(F32)
    lane = lax.broadcasted_iota(jnp.int32, (cap, pixels), 1)
    line_y = jnp.where(lane < half, lane, lane - pixels).astype(F32)
    line_x = jnp.where(lane < half, lane, lane - half).astype(F32)
    norm = 1.0 / (half * half)
    step_angle = 2.0 * math.pi / pixels

    def factors(block, carry):
        rows = pl.ds(pl.multiple_of(block * cap, 8), cap)
        focus, shift_x, shift_y = meta_ref[0, rows], meta_ref[1, rows], meta_ref[2, rows]
        chi_y = math.pi * focus * (line_y * line_y * norm) + DELTA
        chi_x = math.pi * focus * (line_x * line_x * norm)
        phi_y = step_angle * shift_y * line_y
        phi_x = step_angle * shift_x * line_x
        s_y, c_y, p_y, q_y = jnp.sin(chi_y), jnp.cos(chi_y), jnp.cos(phi_y), jnp.sin(phi_y)
        c_x, s_x, p_x, q_x = jnp.cos(chi_x), jnp.sin(chi_x), jnp.cos(phi_x), jnp.sin(phi_x)
        values = (s_y * p_y, s_y * q_y, c_y * p_y, c_y * q_y,
                  c_x * p_x, c_x * q_x, s_x * p_x, s_x * q_x)
        for place, value in enumerate(values):
            factor_ref[rows, place] = value
        return carry

    lax.fori_loop(0, meta_ref.shape[1] // cap, factors, 0)

    def process(refs_ref, owner):
        def pair(step, carry):
            base = owner * cap + step * 2
            both = jnp.concatenate(
                [patch_ref[src_ref[base]], patch_ref[src_ref[base + 1]]], axis=1
            )
            first = jnp.dot(first_ref[...], both, preferred_element_type=F32).astype(BF16)
            for part in range(2):
                slot = base + part
                which = which_ref[slot]
                mine = first[:, part * pixels : (part + 1) * pixels]
                wide = jnp.concatenate([mine[:pixels], mine[pixels:]], axis=1)
                spectrum = jnp.dot(wide, second_ref[...], preferred_element_type=F32)
                line = lax.dot_general(
                    nyq_ref[...], mine, (((1,), (1,)), ((), ())), preferred_element_type=F32
                )
                factor = factor_ref[slot]
                a, b, c, d = factor[4:5], factor[5:6], factor[6:7], factor[7:8]
                cols = factor[0:4]
                rows = jnp.concatenate(
                    [
                        jnp.concatenate([-a, b, -c, d], axis=0),
                        jnp.concatenate([-b, -a, -d, -c], axis=0),
                    ],
                    axis=1,
                )
                col_high = cols.astype(BF16).astype(F32)
                row_high = rows.astype(BF16).astype(F32)
                col_low, row_low = cols - col_high, rows - row_high
                col_all = jnp.concatenate(
                    [col_high, col_high, col_low, jnp.zeros_like(col_low)], axis=0
                ).astype(BF16)
                row_all = jnp.concatenate(
                    [row_high, row_low, row_high, jnp.zeros_like(row_low)], axis=0
                ).astype(BF16)
                turn = lax.dot_general(
                    col_all, row_all, (((0,), (0,)), ((), ())), preferred_element_type=F32
                )
                ref = refs_ref[which, :pixels].astype(F32)
                plain = spectrum[:, :pixels]
                along = plain * ref
                across = spectrum[:, pixels:] * ref
                cosine = turn[:, :pixels]
                sine = turn[:, pixels:]
                real = cosine * along - sine * across
                imag = sine * along + cosine * across
                sums_ref[slot] = jnp.concatenate(
                    [
                        jnp.sum(real, axis=0, keepdims=True),
                        jnp.sum(imag, axis=0, keepdims=True),
                        jnp.sum(imag * freq_y, axis=0, keepdims=True),
                        jnp.sum(plain * plain, axis=0, keepdims=True),
                        plain[half : half + 1],
                        line[0:1, :pixels],
                        line[0:1, pixels:],
                        jnp.zeros((1, pixels), F32),
                    ],
                    axis=0,
                )
                extra_ref[slot] = refs_ref[which, pixels:].astype(F32)
            return carry

        lax.fori_loop(0, cap // 2, pair, 0)

    process(own_ref, me)
    pair_own.wait_recv()
    process(pair_ref, partner)
    for hop in range(1, chips):
        @pl.when(chip >= hop)
        def _():
            to_right(hop - 1).wait_recv()
            if hop < last:
                @pl.when(chip < last)
                def _():
                    to_right(hop).start()
            pair_left(hop - 1).start()

        @pl.when(chip + hop <= last)
        def _():
            to_left(hop - 1).wait_recv()
            if hop < last:
                @pl.when(chip > 0)
                def _():
                    to_left(hop).start()
            pair_right(hop - 1).start()

        @pl.when(chip >= hop)
        def _():
            process(lefts[hop - 1], me - CORES * hop)
            pair_left(hop - 1).wait_recv()
            process(left_pairs[hop - 1], partner - CORES * hop)

        @pl.when(chip + hop <= last)
        def _():
            process(rights[hop - 1], me + CORES * hop)
            pair_right(hop - 1).wait_recv()
            process(right_pairs[hop - 1], partner + CORES * hop)

    pair_own.wait_send()
    for hop in range(last):
        @pl.when((chip >= hop) & (chip < last))
        def _():
            to_right(hop).wait_send()

        @pl.when((chip + hop <= last) & (chip > 0))
        def _():
            to_left(hop).wait_send()

        @pl.when(chip >= hop + 1)
        def _():
            pair_left(hop).wait_send()

        @pl.when(chip + hop + 1 <= last)
        def _():
            pair_right(hop).wait_send()


def gather_sums(cap, src, which, own, patches, meta, first, second, nyquist):
    chips = lax.axis_size("dom") // CORES
    pixels = patches.shape[1]
    padded = src.shape[0]
    vmem = pl.BlockSpec(memory_space=pltpu.VMEM)
    smem = pl.BlockSpec(memory_space=pltpu.SMEM)
    dma = pltpu.SemaphoreType.DMA((chips,))
    return pl.pallas_call(
        functools.partial(gather_kernel, chips, cap),
        out_shape=(
            jax.ShapeDtypeStruct((padded, 8, pixels), F32),
            jax.ShapeDtypeStruct((padded, EXTRA_ROWS, pixels), F32),
        ),
        in_specs=[smem, smem] + [vmem] * 6,
        out_specs=(vmem, vmem),
        scratch_shapes=[pltpu.VMEM((padded, 8, pixels), F32)]
        + [pltpu.VMEM(own.shape, own.dtype)] * (4 * (chips - 1) + 1)
        + [dma] * 8
        + [pltpu.SemaphoreType.DMA] * 2,
        compiler_params=pltpu.CompilerParams(
            collective_id=0, has_side_effects=True, vmem_limit_bytes=56 * 1024 * 1024
        ),
        name="gather_sums",
    )(src, which, own, patches, meta, first, second, nyquist)


def step_kernel(owners, grad_ref, warp_ref, out_ref, held_ref, send_sem, recv_sem):
    me = lax.axis_index("dom")
    barrier = pltpu.get_barrier_semaphore()
    for hop in range(1, owners):
        pl.semaphore_signal(
            barrier, inc=1, device_id={"dom": lax.rem(me + hop, owners)},
            device_id_type=pl.DeviceIdType.MESH,
        )
    pl.semaphore_wait(barrier, owners - 1)

    def copy(hop):
        return pltpu.make_async_remote_copy(
            src_ref=grad_ref, dst_ref=held_ref.at[hop - 1], send_sem=send_sem.at[hop - 1],
            recv_sem=recv_sem.at[hop - 1], device_id={"dom": lax.rem(me + hop, owners)},
            device_id_type=pl.DeviceIdType.MESH,
        )

    for hop in range(1, owners):
        copy(hop).start()
    for hop in range(1, owners):
        copy(hop).wait()
    total = grad_ref[...]
    for hop in range(1, owners):
        total = total + held_ref[hop - 1]
    out_ref[...] = warp_ref[...] - total / jnp.sqrt(total * total + TRUST_FLOOR * TRUST_FLOOR)


def warp_step(gradient, warp):
    owners = lax.axis_size("dom")
    vmem = pl.BlockSpec(memory_space=pltpu.VMEM)
    dma = pltpu.SemaphoreType.DMA((owners - 1,))
    return pl.pallas_call(
        functools.partial(step_kernel, owners),
        out_shape=jax.ShapeDtypeStruct(warp.shape, F32),
        in_specs=[vmem, vmem],
        out_specs=vmem,
        scratch_shapes=[pltpu.VMEM((owners - 1,) + warp.shape, F32), dma, dma],
        compiler_params=pltpu.CompilerParams(collective_id=1, has_side_effects=True),
        name="warp_step",
    )(gradient, warp)


def pass_tables(pixels):
    half = pixels // 2
    row_table, col_table = dft_tables(jnp.arange(pixels, dtype=jnp.int32), pixels)
    cosine = col_table[:, :half]
    sine = col_table[:, pixels : pixels + half]
    real = jnp.concatenate([cosine, -sine], axis=0)
    imag = jnp.concatenate([-sine, -cosine], axis=0)
    second = jnp.concatenate([real, imag, imag, -real], axis=1)
    nyquist = jnp.broadcast_to(col_table[:, half][None, :], (16, pixels))
    return row_table, second, nyquist


def line_terms(spec_re, spec_im, ref_re, ref_im, chi, phi):
    contrast = -jnp.sin(chi + DELTA)
    cosine = jnp.cos(phi)
    sine = jnp.sin(phi)
    model_re = contrast * (ref_re * cosine + ref_im * sine)
    model_im = contrast * (ref_im * cosine - ref_re * sine)
    return spec_re * model_re + spec_im * model_im, spec_im * model_re - spec_re * model_im


def finish_terms(sums, extra, focus, shifts, pixels):
    half = pixels // 2
    k = jnp.arange(pixels, dtype=jnp.int32)
    freq = signed_freq(k, pixels)
    lane_freq = (k % half).astype(F32)
    step = 2.0 * math.pi / pixels
    norm = 1.0 / (half * half)
    match = jnp.sum(sums[:, 0], axis=1)
    grad_x = jnp.sum(sums[:, 1] * lane_freq, axis=1)
    grad_y = jnp.sum(sums[:, 2], axis=1)
    power = jnp.sum(sums[:, 3] * jnp.where(lane_freq > 0, 2.0, 1.0), axis=1)
    d = focus[:, None]
    s_x, s_y = shifts[:, 0:1], shifts[:, 1:2]
    col_re, col_im = sums[:, 5], -sums[:, 6]
    power = power + jnp.sum(col_re * col_re + col_im * col_im, axis=1)
    along, across = line_terms(
        col_re, col_im, extra[:, 0], extra[:, 1],
        math.pi * d * (freq * freq * norm + 1.0), step * (freq * s_y - half * s_x),
    )
    match = match + jnp.sum(along, axis=1)
    grad_x = grad_x - half * jnp.sum(across, axis=1)
    grad_y = grad_y + jnp.sum(across * freq, axis=1)
    f = lane_freq[:half]
    along, across = line_terms(
        sums[:, 4, :half], -sums[:, 4, half:], extra[:, 2, :half], extra[:, 2, half:],
        math.pi * d * (f * f * norm + 1.0), step * (-f * s_x - half * s_y),
    )
    match = match + jnp.sum(along, axis=1)
    grad_x = grad_x - jnp.sum(across * f, axis=1)
    grad_y = grad_y - half * jnp.sum(across, axis=1)
    place = jnp.where(
        focus < 2.0, (focus - 1.0) * pixels, pixels + (focus - 2.0) * half
    )
    table_high = extra[:, 3:5].reshape(-1, 2 * pixels)
    table_low = extra[:, 5:7].reshape(-1, 2 * pixels)
    hit = place[:, None] == jnp.arange(2 * pixels, dtype=jnp.int32).astype(F32)[None, :]
    model_power = jnp.sum(jnp.where(hit, table_high + table_low, 0.0), axis=1)
    area = 1.0 / (pixels * pixels)
    energy = (power + model_power - 2.0 * match) * area
    return jnp.stack([energy, 2.0 * area * step * grad_x, 2.0 * area * step * grad_y], axis=0)


def on_device_gathered(
    patches, slot_view, slot_tilt, slot_pos, defocus, projections, warp_grid
):
    owners = lax.axis_size("dom")
    pixels = patches.shape[-1]
    slots = patches.shape[1]
    view_dev = projections.shape[0]
    tilt_dev = warp_grid.shape[0]
    node_count = warp_grid.shape[2]
    cap = 3 * slots // (2 * owners)
    padded = owners * cap
    exact = functools.partial(
        jnp.dot, precision=lax.Precision.HIGHEST, preferred_element_type=F32
    )
    own = fold_references(projections, pixels)
    tilt = slot_tilt[0]
    view = slot_view[0, :, 0]
    slot_iota = jnp.arange(slots, dtype=jnp.int32)
    owner_of = view // view_dev
    ahead = (owner_of[:, None] == owner_of[None, :]) & (slot_iota[None, :] < slot_iota[:, None])
    target = owner_of * cap + jnp.sum(ahead.astype(jnp.int32), axis=1)
    matches = (target[None, :] == jnp.arange(padded, dtype=jnp.int32)[:, None]).astype(F32)
    weights = node_weights(slot_pos[0, 0].astype(F32), slot_pos[1, 0].astype(F32), GRID)
    tilt_match = (tilt[:, None] == jnp.arange(tilt_dev, dtype=jnp.int32)[None, :]).astype(F32)
    chosen = exact(tilt_match, warp_grid.reshape(tilt_dev, -1))
    shift_x = jnp.sum(chosen[:, :node_count] * weights, axis=1)
    shift_y = jnp.sum(chosen[:, node_count:] * weights, axis=1)
    facts = jnp.stack(
        [
            slot_iota.astype(F32),
            ((view % view_dev) * tilt_dev + tilt).astype(F32),
            defocus[0].astype(F32),
            shift_x,
            shift_y,
        ],
        axis=1,
    )
    facts = exact(matches, facts)
    src = jnp.round(facts[:, 0]).astype(jnp.int32)
    which = jnp.round(facts[:, 1]).astype(jnp.int32)
    focus = facts[:, 2]
    shifts = facts[:, 3:5]
    meta = jnp.broadcast_to(facts[:, 2:5].T[:, :, None], (3, padded, pixels))
    first, second, nyquist = pass_tables(pixels)
    sums, extra = gather_sums(cap, src, which, own, patches[0], meta, first, second, nyquist)
    terms = exact(finish_terms(sums, extra, focus, shifts, pixels), matches)
    coef = (tilt_match.T[:, None, :] * terms[None, 1:3, :]).reshape(2 * tilt_dev, -1)
    gradient = exact(coef, weights).reshape(tilt_dev, 2 * node_count)
    new_warp = warp_step(gradient, warp_grid.reshape(tilt_dev, 2 * node_count))
    return (terms[:, None, :], new_warp.reshape(warp_grid.shape))


def solution(mesh):
    body = on_device if mesh.shape["rep"] > 1 else on_device_gathered
    in_specs = (
        P(("groups", "tilt"), "dom", None, None),
        P(("groups", "tilt"), "dom", None),
        P(("groups", "tilt"), "dom"),
        P(None, ("groups", "tilt"), "dom"),
        P(("groups", "tilt"), "dom"),
        P(("groups", "dom"), "tilt", None, "rep", None),
        P(("groups", "tilt"), None, None),
    )
    out_specs = (P(None, ("groups", "tilt"), "dom"), P(("groups", "tilt"), None, None))
    return jax.shard_map(
        body, mesh=mesh, in_specs=in_specs, out_specs=out_specs, check_vma=False
    )
```

```python
import functools
import math

import jax
import jax.numpy as jnp
from jax import lax
from jax.experimental import pallas as pl
from jax.experimental.pallas import tpu as pltpu
from jax.sharding import PartitionSpec as P

GRID = 16


AMPLITUDE = 0.07
TRUST_FLOOR = 0.02


def signed_freq(index, pixels):
    return jnp.where(index < pixels // 2, index, index - pixels).astype(jnp.float32)


def dft_tables(freq_rows, pixels):
    columns = jnp.arange(pixels, dtype=jnp.int32)
    table_scale = 1.0 / math.sqrt(pixels)
    turns_rows = (freq_rows[:, None] * columns[None, :] % pixels).astype(jnp.float32) * (
        2.0 * math.pi / pixels
    )
    turns_full = (columns[:, None] * columns[None, :] % pixels).astype(jnp.float32) * (
        2.0 * math.pi / pixels
    )
    row_table = jnp.concatenate([jnp.cos(turns_rows), jnp.sin(turns_rows)], axis=0) * table_scale
    col_table = jnp.concatenate([jnp.cos(turns_full), jnp.sin(turns_full)], axis=1) * table_scale
    return (row_table.astype(jnp.bfloat16), col_table.astype(jnp.bfloat16))


def node_weights(pos_x, pos_y, grid_side):
    knot_pos = jnp.arange(grid_side, dtype=jnp.int32).astype(jnp.float32)
    weight_x = jnp.maximum(0.0, 1.0 - jnp.abs(pos_x[:, None] * (grid_side - 1) - knot_pos[None, :]))
    weight_y = jnp.maximum(0.0, 1.0 - jnp.abs(pos_y[:, None] * (grid_side - 1) - knot_pos[None, :]))
    return (weight_y[:, :, None] * weight_x[:, None, :]).reshape(
        pos_x.shape[0], grid_side * grid_side
    )


def spectral_terms(spectrum, ref_blk, focus_blk, shift_blk, freq_rows, pixels):
    row_total = freq_rows.shape[0]
    v_one_cos = spectrum[:, :row_total, :pixels]
    v_one_sin = spectrum[:, :row_total, pixels:]
    v_two_cos = spectrum[:, row_total:, :pixels]
    v_two_sin = spectrum[:, row_total:, pixels:]
    real_part = v_one_cos - v_two_sin
    imag_part = -(v_one_sin + v_two_cos)
    freq_y = signed_freq(freq_rows, pixels)[None, :, None]
    freq_x = signed_freq(jnp.arange(pixels, dtype=jnp.int32), pixels)[None, None, :]
    nyquist = pixels / 2.0
    radius = (freq_y * freq_y + freq_x * freq_x) / (nyquist * nyquist)
    aberration = math.pi * focus_blk[:, None, None] * radius
    contrast = -(
        math.sqrt(1.0 - AMPLITUDE * AMPLITUDE) * jnp.sin(aberration)
        + AMPLITUDE * jnp.cos(aberration)
    )
    phase_angle = (
        2.0
        * math.pi
        / pixels
        * (freq_x * shift_blk[:, 0, None, None] + freq_y * shift_blk[:, 1, None, None])
    )
    cosine = jnp.cos(phase_angle)
    sine_part = jnp.sin(phase_angle)
    ref_real = ref_blk[:, 0].astype(jnp.float32)
    ref_imag = ref_blk[:, 1].astype(jnp.float32)
    model_real = contrast * (ref_real * cosine + ref_imag * sine_part)
    model_imag = contrast * (ref_imag * cosine - ref_real * sine_part)
    diff_real = real_part - model_real
    diff_imag = imag_part - model_imag
    inverse_area = 1.0 / (pixels * pixels)
    energy = jnp.sum(diff_real * diff_real + diff_imag * diff_imag, axis=(1, 2)) * inverse_area
    cross_term = diff_imag * model_real - diff_real * model_imag
    grad_x = 2.0 * inverse_area * jnp.sum(2.0 * math.pi / pixels * freq_x * cross_term, axis=(1, 2))
    grad_y = 2.0 * inverse_area * jnp.sum(2.0 * math.pi / pixels * freq_y * cross_term, axis=(1, 2))
    return jnp.stack([energy, grad_x, grad_y], axis=1)


def on_device(patches, slot_view, slot_tilt, slot_pos, defocus, projections, warp_grid):
    owners = lax.axis_size("dom")
    slot_count = patches.shape[1]
    pixels = patches.shape[-1]
    view_dev = projections.shape[0]
    tilt_dev = warp_grid.shape[0]
    node_count = warp_grid.shape[2]
    capacity = 3 * slot_count // (2 * owners)
    buffer_len = owners * capacity
    chosen_view = slot_view[0, :, 0]
    owner_of = chosen_view // view_dev
    owner_hits = (owner_of[:, None] == jnp.arange(owners, dtype=jnp.int32)[None, :]).astype(
        jnp.int32
    )
    earlier = jnp.cumsum(owner_hits, axis=0) - owner_hits
    slot_rank = jnp.sum(earlier * owner_hits, axis=1)
    target = owner_of * capacity + slot_rank
    matches = target[None, :] == jnp.arange(buffer_len, dtype=jnp.int32)[:, None]
    source = jnp.sum(
        jnp.where(matches, jnp.arange(slot_count, dtype=jnp.int32)[None, :], 0), axis=1
    )
    filled = jnp.any(matches, axis=1)
    patch_rows = jnp.where(filled[:, None, None], patches[0][source], jnp.zeros((), jnp.bfloat16))
    slot_meta = jnp.stack(
        [
            slot_tilt[0].astype(jnp.float32),
            (chosen_view % view_dev).astype(jnp.float32),
            defocus[0].astype(jnp.float32),
            slot_pos[0, 0].astype(jnp.float32),
            slot_pos[1, 0].astype(jnp.float32),
            jnp.ones((slot_count,), jnp.float32),
        ],
        axis=1,
    )
    meta_rows = jnp.where(filled[:, None], slot_meta[source], 0.0).astype(jnp.bfloat16)
    patch_buffer = patch_rows.reshape(owners, capacity, pixels, pixels)
    meta_buffer = meta_rows.reshape(owners, capacity, 6)
    row_span = projections.shape[3]
    freq_rows = lax.axis_index("rep") * row_span + jnp.arange(row_span, dtype=jnp.int32)
    row_table, col_table = dft_tables(freq_rows, pixels)
    row_total = freq_rows.shape[0]
    projected_flat = projections.reshape(view_dev * tilt_dev, 2, row_total, pixels)
    tilt_iota = jnp.arange(tilt_dev, dtype=jnp.int32)
    view_iota = jnp.arange(view_dev, dtype=jnp.int32)

    def one_block(inputs):
        patch_blk, index_blk, focus_blk, shift_blk = inputs
        ref_blk = projected_flat[index_blk]
        first_pass = jnp.einsum(
            "fy,byx->bfx", row_table, patch_blk, preferred_element_type=jnp.float32
        ).astype(jnp.bfloat16)
        spectrum = jnp.einsum(
            "bfx,xk->bfk", first_pass, col_table, preferred_element_type=jnp.float32
        )
        return spectral_terms(spectrum, ref_blk, focus_blk, shift_blk, freq_rows, pixels)

    patch_in = lax.all_to_all(patch_buffer, "dom", split_axis=0, concat_axis=0, tiled=True)
    meta_in = lax.all_to_all(meta_buffer, "dom", split_axis=0, concat_axis=0, tiled=True)
    senders = patch_in.shape[0]
    per_sender = patch_in.shape[1]
    slot_total = senders * per_sender
    meta_flat = meta_in.reshape(slot_total, 6).astype(jnp.float32)
    tilt_match = meta_flat[:, 0:1] == tilt_iota.astype(jnp.float32)[None, :]
    view_match = meta_flat[:, 1:2] == view_iota.astype(jnp.float32)[None, :]
    tilt_local = jnp.sum(jnp.where(tilt_match, tilt_iota[None, :], 0), axis=1)
    view_local = jnp.sum(jnp.where(view_match, view_iota[None, :], 0), axis=1)
    weights = node_weights(meta_flat[:, 3], meta_flat[:, 4], GRID)
    shifts = jnp.sum(warp_grid[tilt_local] * weights[:, None, :], axis=2)
    block_len = math.gcd(slot_total, 16)
    block_count = slot_total // block_len
    per_slot = lax.map(
        one_block,
        (
            patch_in.reshape(block_count, block_len, pixels, pixels),
            (view_local * tilt_dev + tilt_local).reshape(block_count, block_len),
            meta_flat[:, 2].reshape(block_count, block_len),
            shifts.reshape(block_count, block_len, 2),
        ),
    ).reshape(slot_total, 3)
    node_coef = (
        tilt_match.astype(jnp.float32)[:, :, None]
        * per_slot[:, None, 1:3]
        * meta_flat[:, 5, None, None]
    ).reshape(senders, per_sender, 2 * tilt_dev)
    returned = lax.all_to_all(
        per_slot.reshape(senders, per_sender, 3), "dom", split_axis=0, concat_axis=0, tiled=True
    )
    weight_all = weights.reshape(senders, per_sender, node_count)
    own_terms = returned.reshape(buffer_len, 3)[target]
    summed = lax.psum(own_terms, "rep")
    slot_terms = summed.T[:, None, :]
    gradient = jnp.dot(
        node_coef.reshape(-1, 2 * tilt_dev).T,
        weight_all.reshape(-1, node_count),
        precision=lax.Precision.HIGHEST,
        preferred_element_type=jnp.float32,
    ).reshape(tilt_dev, 2, node_count)
    whole_grad = lax.psum(gradient, ("dom", "rep"))
    new_warp = warp_grid - whole_grad / jnp.sqrt(
        whole_grad * whole_grad + TRUST_FLOOR * TRUST_FLOOR
    )
    return (slot_terms, new_warp)


CORES = 2
EXTRA_ROWS = 8
DELTA = math.asin(AMPLITUDE)
F32 = jnp.float32
BF16 = jnp.bfloat16


def fold_kernel(refs_ref, pick_ref, turn_ref, unit_ref, waves_ref, weights_ref, out_ref):
    pixels = turn_ref.shape[0]
    half = pixels // 2
    lane = lax.broadcasted_iota(jnp.int32, (1, pixels), 1)
    sign = jnp.where(lane < half, 1.0, -1.0)

    def one(n, carry):
        real, imag = refs_ref[n, 0], refs_ref[n, 1]
        wide = jnp.concatenate([real, imag], axis=1)
        picked = jnp.dot(wide, pick_ref[...], preferred_element_type=F32)
        mirrored = picked[:, pixels:]
        turned = jnp.dot(turn_ref[...], mirrored.astype(BF16), preferred_element_type=F32)
        out_ref[n, :pixels] = (picked[:, :pixels] + sign * turned).astype(BF16)
        tall = jnp.concatenate([real, imag], axis=0)
        column = lax.dot_general(
            unit_ref[...], tall, (((1,), (1,)), ((), ())), preferred_element_type=F32
        )
        r, i = real.astype(F32), imag.astype(F32)
        power = r * r + i * i
        mixed = jnp.dot(power.astype(BF16), waves_ref[...], preferred_element_type=F32)
        swing = jnp.sum(mixed * weights_ref[...], axis=0, keepdims=True)
        swing = swing[:, : 2 * pixels] + swing[:, 2 * pixels :]
        total = 0.5 * jnp.sum(power) - 0.5 * swing
        high = total.astype(BF16).astype(F32)
        low = total - high
        extra = jnp.concatenate(
            [
                column[0:1, :pixels],
                column[0:1, pixels:],
                mirrored[half : half + 1],
                high[:, :pixels],
                high[:, pixels:],
                low[:, :pixels],
                low[:, pixels:],
                jnp.zeros((EXTRA_ROWS - 7, pixels), F32),
            ],
            axis=0,
        )
        out_ref[n, pixels:] = extra.astype(BF16)
        return carry

    lax.fori_loop(0, refs_ref.shape[0], one, 0, unroll=True)


def fold_references(projections, pixels):
    half = pixels // 2
    refs = projections.reshape(-1, 2, pixels, pixels)
    count = refs.shape[0]
    k = jnp.arange(pixels, dtype=jnp.int32)
    lane_freq = k % half
    lane_part = k // half
    chan = jnp.arange(2, dtype=jnp.int32)
    same_part = chan[:, None, None] == lane_part[None, None, :]
    pick = same_part & (k[None, :, None] == lane_freq[None, None, :])
    flip = (
        same_part
        & (k[None, :, None] == pixels - lane_freq[None, None, :])
        & (lane_freq > 0)[None, None, :]
    )
    picks = jnp.concatenate([pick, flip], axis=2).reshape(2 * pixels, 2 * pixels).astype(BF16)
    turn = (((k[:, None] + k[None, :]) % pixels == 0) & (k != half)[:, None]).astype(BF16)
    unit = jnp.broadcast_to((k == half).astype(BF16)[None, :], (16, pixels))
    table = jnp.arange(2 * pixels, dtype=jnp.int32)
    focus = jnp.where(
        table < pixels, 1.0 + table / pixels, 2.0 + (table - pixels) / (pixels // 2)
    ).astype(F32)
    freq = signed_freq(k, pixels)
    chi = math.pi * focus[None, :] * (freq * freq / (half * half))[:, None]
    chi = jnp.concatenate([chi, chi + 0.25 * math.pi], axis=1) * 2.0
    waves = jnp.cos(jnp.concatenate([chi[:, : 2 * pixels], chi[:, 2 * pixels :] - math.pi], axis=1))
    weights = jnp.cos(chi + 2.0 * DELTA)
    rows = pixels + EXTRA_ROWS
    group = math.gcd(count, 5)
    full = lambda x: pl.BlockSpec(x.shape, lambda i: (0, 0))
    tables = (picks, turn, unit, waves.astype(BF16), weights)
    return pl.pallas_call(
        fold_kernel,
        grid=(count // group,),
        out_shape=jax.ShapeDtypeStruct((count, rows, pixels), BF16),
        in_specs=[pl.BlockSpec((group, 2, pixels, pixels), lambda i: (i, 0, 0, 0))]
        + [full(x) for x in tables],
        out_specs=pl.BlockSpec((group, rows, pixels), lambda i: (i, 0, 0)),
        name="fold_references",
    )(refs, *tables)


def gather_kernel(chips, cap, src_ref, which_ref, own_ref, patch_ref, meta_ref, first_ref,
                  second_ref, nyq_ref, sums_ref, extra_ref, factor_ref, *rest):
    lefts, rights = rest[: chips - 1], rest[chips - 1 : 2 * chips - 2]
    left_pairs, right_pairs = rest[2 * chips - 2 : 3 * chips - 3], rest[3 * chips - 3 : 4 * chips - 4]
    (pair_ref, rs, rr, ls, lr, lps, lpr, rps, rpr, ps, pr) = rest[4 * chips - 4 :]
    pixels = patch_ref.shape[1]
    half = pixels // 2
    me = lax.axis_index("dom")
    chip = me // CORES
    core = me % CORES
    partner = chip * CORES + (1 - core)
    right = me + CORES
    left = me - CORES
    last = chips - 1
    barrier = pltpu.get_barrier_semaphore()

    def greet(device):
        pl.semaphore_signal(
            barrier, inc=1, device_id={"dom": device}, device_id_type=pl.DeviceIdType.MESH
        )

    greet(partner)

    @pl.when(chip < last)
    def _():
        greet(right)

    @pl.when(chip > 0)
    def _():
        greet(left)

    inner = (chip > 0) & (chip < last)

    @pl.when(inner)
    def _():
        pl.semaphore_wait(barrier, 3)

    @pl.when(jnp.logical_not(inner))
    def _():
        pl.semaphore_wait(barrier, 2)

    def copy(src, dst, send, recv, target):
        return pltpu.make_async_remote_copy(
            src_ref=src, dst_ref=dst, send_sem=send, recv_sem=recv,
            device_id={"dom": target}, device_id_type=pl.DeviceIdType.MESH,
        )

    def to_right(hop):
        src = own_ref if hop == 0 else lefts[hop - 1]
        return copy(src, lefts[hop], rs.at[hop], rr.at[hop], right)

    def to_left(hop):
        src = own_ref if hop == 0 else rights[hop - 1]
        return copy(src, rights[hop], ls.at[hop], lr.at[hop], left)

    def pair_left(hop):
        return copy(lefts[hop], left_pairs[hop], lps.at[hop], lpr.at[hop], partner)

    def pair_right(hop):
        return copy(rights[hop], right_pairs[hop], rps.at[hop], rpr.at[hop], partner)

    pair_own = copy(own_ref, pair_ref, ps, pr, partner)

    @pl.when(chip < last)
    def _():
        to_right(0).start()

    @pl.when(chip > 0)
    def _():
        to_left(0).start()

    pair_own.start()

    row_index = lax.broadcasted_iota(jnp.int32, (pixels, pixels), 0)
    freq_y = jnp.where(row_index < half, row_index, row_index - pixels).astype(F32)
    lane = lax.broadcasted_iota(jnp.int32, (cap, pixels), 1)
    line_y = jnp.where(lane < half, lane, lane - pixels).astype(F32)
    line_x = jnp.where(lane < half, lane, lane - half).astype(F32)
    norm = 1.0 / (half * half)
    step_angle = 2.0 * math.pi / pixels

    def factors(block, carry):
        rows = pl.ds(pl.multiple_of(block * cap, 8), cap)
        focus, shift_x, shift_y = meta_ref[0, rows], meta_ref[1, rows], meta_ref[2, rows]
        chi_y = math.pi * focus * (line_y * line_y * norm) + DELTA
        chi_x = math.pi * focus * (line_x * line_x * norm)
        phi_y = step_angle * shift_y * line_y
        phi_x = step_angle * shift_x * line_x
        s_y, c_y, p_y, q_y = jnp.sin(chi_y), jnp.cos(chi_y), jnp.cos(phi_y), jnp.sin(phi_y)
        c_x, s_x, p_x, q_x = jnp.cos(chi_x), jnp.sin(chi_x), jnp.cos(phi_x), jnp.sin(phi_x)
        values = (s_y * p_y, s_y * q_y, c_y * p_y, c_y * q_y,
                  c_x * p_x, c_x * q_x, s_x * p_x, s_x * q_x)
        for place, value in enumerate(values):
            factor_ref[rows, place] = value
        return carry

    lax.fori_loop(0, meta_ref.shape[1] // cap, factors, 0)

    def process(refs_ref, owner):
        def pair(step, carry):
            base = owner * cap + step * 2
            both = jnp.concatenate(
                [patch_ref[src_ref[base]], patch_ref[src_ref[base + 1]]], axis=1
            )
            first = jnp.dot(first_ref[...], both, preferred_element_type=F32).astype(BF16)
            for part in range(2):
                slot = base + part
                which = which_ref[slot]
                mine = first[:, part * pixels : (part + 1) * pixels]
                wide = jnp.concatenate([mine[:pixels], mine[pixels:]], axis=1)
                spectrum = jnp.dot(wide, second_ref[...], preferred_element_type=F32)
                line = lax.dot_general(
                    nyq_ref[...], mine, (((1,), (1,)), ((), ())), preferred_element_type=F32
                )
                factor = factor_ref[slot]
                a, b, c, d = factor[4:5], factor[5:6], factor[6:7], factor[7:8]
                cols = factor[0:4]
                rows = jnp.concatenate(
                    [
                        jnp.concatenate([-a, b, -c, d], axis=0),
                        jnp.concatenate([-b, -a, -d, -c], axis=0),
                    ],
                    axis=1,
                )
                col_high = cols.astype(BF16).astype(F32)
                row_high = rows.astype(BF16).astype(F32)
                col_low, row_low = cols - col_high, rows - row_high
                col_all = jnp.concatenate(
                    [col_high, col_high, col_low, jnp.zeros_like(col_low)], axis=0
                ).astype(BF16)
                row_all = jnp.concatenate(
                    [row_high, row_low, row_high, jnp.zeros_like(row_low)], axis=0
                ).astype(BF16)
                turn = lax.dot_general(
                    col_all, row_all, (((0,), (0,)), ((), ())), preferred_element_type=F32
                )
                ref = refs_ref[which, :pixels].astype(F32)
                plain = spectrum[:, :pixels]
                along = plain * ref
                across = spectrum[:, pixels:] * ref
                cosine = turn[:, :pixels]
                sine = turn[:, pixels:]
                real = cosine * along - sine * across
                imag = sine * along + cosine * across
                sums_ref[slot] = jnp.concatenate(
                    [
                        jnp.sum(real, axis=0, keepdims=True),
                        jnp.sum(imag, axis=0, keepdims=True),
                        jnp.sum(imag * freq_y, axis=0, keepdims=True),
                        jnp.sum(plain * plain, axis=0, keepdims=True),
                        plain[half : half + 1],
                        line[0:1, :pixels],
                        line[0:1, pixels:],
                        jnp.zeros((1, pixels), F32),
                    ],
                    axis=0,
                )
                extra_ref[slot] = refs_ref[which, pixels:].astype(F32)
            return carry

        lax.fori_loop(0, cap // 2, pair, 0)

    process(own_ref, me)
    pair_own.wait_recv()
    process(pair_ref, partner)
    for hop in range(1, chips):
        @pl.when(chip >= hop)
        def _():
            to_right(hop - 1).wait_recv()
            if hop < last:
                @pl.when(chip < last)
                def _():
                    to_right(hop).start()
            pair_left(hop - 1).start()

        @pl.when(chip + hop <= last)
        def _():
            to_left(hop - 1).wait_recv()
            if hop < last:
                @pl.when(chip > 0)
                def _():
                    to_left(hop).start()
            pair_right(hop - 1).start()

        @pl.when(chip >= hop)
        def _():
            process(lefts[hop - 1], me - CORES * hop)
            pair_left(hop - 1).wait_recv()
            process(left_pairs[hop - 1], partner - CORES * hop)

        @pl.when(chip + hop <= last)
        def _():
            process(rights[hop - 1], me + CORES * hop)
            pair_right(hop - 1).wait_recv()
            process(right_pairs[hop - 1], partner + CORES * hop)

    pair_own.wait_send()
    for hop in range(last):
        @pl.when((chip >= hop) & (chip < last))
        def _():
            to_right(hop).wait_send()

        @pl.when((chip + hop <= last) & (chip > 0))
        def _():
            to_left(hop).wait_send()

        @pl.when(chip >= hop + 1)
        def _():
            pair_left(hop).wait_send()

        @pl.when(chip + hop + 1 <= last)
        def _():
            pair_right(hop).wait_send()


def gather_sums(cap, src, which, own, patches, meta, first, second, nyquist):
    chips = lax.axis_size("dom") // CORES
    pixels = patches.shape[1]
    padded = src.shape[0]
    vmem = pl.BlockSpec(memory_space=pltpu.VMEM)
    smem = pl.BlockSpec(memory_space=pltpu.SMEM)
    dma = pltpu.SemaphoreType.DMA((chips,))
    return pl.pallas_call(
        functools.partial(gather_kernel, chips, cap),
        out_shape=(
            jax.ShapeDtypeStruct((padded, 8, pixels), F32),
            jax.ShapeDtypeStruct((padded, EXTRA_ROWS, pixels), F32),
        ),
        in_specs=[smem, smem] + [vmem] * 6,
        out_specs=(vmem, vmem),
        scratch_shapes=[pltpu.VMEM((padded, 8, pixels), F32)]
        + [pltpu.VMEM(own.shape, own.dtype)] * (4 * (chips - 1) + 1)
        + [dma] * 8
        + [pltpu.SemaphoreType.DMA] * 2,
        compiler_params=pltpu.CompilerParams(
            collective_id=0, has_side_effects=True, vmem_limit_bytes=56 * 1024 * 1024
        ),
        name="gather_sums",
    )(src, which, own, patches, meta, first, second, nyquist)


def step_kernel(owners, grad_ref, warp_ref, out_ref, held_ref, send_sem, recv_sem):
    me = lax.axis_index("dom")
    barrier = pltpu.get_barrier_semaphore()
    for hop in range(1, owners):
        pl.semaphore_signal(
            barrier, inc=1, device_id={"dom": lax.rem(me + hop, owners)},
            device_id_type=pl.DeviceIdType.MESH,
        )
    pl.semaphore_wait(barrier, owners - 1)

    def copy(hop):
        return pltpu.make_async_remote_copy(
            src_ref=grad_ref, dst_ref=held_ref.at[hop - 1], send_sem=send_sem.at[hop - 1],
            recv_sem=recv_sem.at[hop - 1], device_id={"dom": lax.rem(me + hop, owners)},
            device_id_type=pl.DeviceIdType.MESH,
        )

    for hop in range(1, owners):
        copy(hop).start()
    for hop in range(1, owners):
        copy(hop).wait()
    total = grad_ref[...]
    for hop in range(1, owners):
        total = total + held_ref[hop - 1]
    out_ref[...] = warp_ref[...] - total / jnp.sqrt(total * total + TRUST_FLOOR * TRUST_FLOOR)


def warp_step(gradient, warp):
    owners = lax.axis_size("dom")
    vmem = pl.BlockSpec(memory_space=pltpu.VMEM)
    dma = pltpu.SemaphoreType.DMA((owners - 1,))
    return pl.pallas_call(
        functools.partial(step_kernel, owners),
        out_shape=jax.ShapeDtypeStruct(warp.shape, F32),
        in_specs=[vmem, vmem],
        out_specs=vmem,
        scratch_shapes=[pltpu.VMEM((owners - 1,) + warp.shape, F32), dma, dma],
        compiler_params=pltpu.CompilerParams(collective_id=1, has_side_effects=True),
        name="warp_step",
    )(gradient, warp)


def pass_tables(pixels):
    half = pixels // 2
    row_table, col_table = dft_tables(jnp.arange(pixels, dtype=jnp.int32), pixels)
    cosine = col_table[:, :half]
    sine = col_table[:, pixels : pixels + half]
    real = jnp.concatenate([cosine, -sine], axis=0)
    imag = jnp.concatenate([-sine, -cosine], axis=0)
    second = jnp.concatenate([real, imag, imag, -real], axis=1)
    nyquist = jnp.broadcast_to(col_table[:, half][None, :], (16, pixels))
    return row_table, second, nyquist


def line_terms(spec_re, spec_im, ref_re, ref_im, chi, phi):
    contrast = -jnp.sin(chi + DELTA)
    cosine = jnp.cos(phi)
    sine = jnp.sin(phi)
    model_re = contrast * (ref_re * cosine + ref_im * sine)
    model_im = contrast * (ref_im * cosine - ref_re * sine)
    return spec_re * model_re + spec_im * model_im, spec_im * model_re - spec_re * model_im


def finish_terms(sums, extra, focus, shifts, pixels):
    half = pixels // 2
    k = jnp.arange(pixels, dtype=jnp.int32)
    freq = signed_freq(k, pixels)
    lane_freq = (k % half).astype(F32)
    step = 2.0 * math.pi / pixels
    norm = 1.0 / (half * half)
    match = jnp.sum(sums[:, 0], axis=1)
    grad_x = jnp.sum(sums[:, 1] * lane_freq, axis=1)
    grad_y = jnp.sum(sums[:, 2], axis=1)
    power = jnp.sum(sums[:, 3] * jnp.where(lane_freq > 0, 2.0, 1.0), axis=1)
    d = focus[:, None]
    s_x, s_y = shifts[:, 0:1], shifts[:, 1:2]
    col_re, col_im = sums[:, 5], -sums[:, 6]
    power = power + jnp.sum(col_re * col_re + col_im * col_im, axis=1)
    along, across = line_terms(
        col_re, col_im, extra[:, 0], extra[:, 1],
        math.pi * d * (freq * freq * norm + 1.0), step * (freq * s_y - half * s_x),
    )
    match = match + jnp.sum(along, axis=1)
    grad_x = grad_x - half * jnp.sum(across, axis=1)
    grad_y = grad_y + jnp.sum(across * freq, axis=1)
    f = lane_freq[:half]
    along, across = line_terms(
        sums[:, 4, :half], -sums[:, 4, half:], extra[:, 2, :half], extra[:, 2, half:],
        math.pi * d * (f * f * norm + 1.0), step * (-f * s_x - half * s_y),
    )
    match = match + jnp.sum(along, axis=1)
    grad_x = grad_x - jnp.sum(across * f, axis=1)
    grad_y = grad_y - half * jnp.sum(across, axis=1)
    place = jnp.where(
        focus < 2.0, (focus - 1.0) * pixels, pixels + (focus - 2.0) * half
    )
    table_high = extra[:, 3:5].reshape(-1, 2 * pixels)
    table_low = extra[:, 5:7].reshape(-1, 2 * pixels)
    hit = place[:, None] == jnp.arange(2 * pixels, dtype=jnp.int32).astype(F32)[None, :]
    model_power = jnp.sum(jnp.where(hit, table_high + table_low, 0.0), axis=1)
    area = 1.0 / (pixels * pixels)
    energy = (power + model_power - 2.0 * match) * area
    return jnp.stack([energy, 2.0 * area * step * grad_x, 2.0 * area * step * grad_y], axis=0)


def on_device_gathered(
    patches, slot_view, slot_tilt, slot_pos, defocus, projections, warp_grid
):
    owners = lax.axis_size("dom")
    pixels = patches.shape[-1]
    slots = patches.shape[1]
    view_dev = projections.shape[0]
    tilt_dev = warp_grid.shape[0]
    node_count = warp_grid.shape[2]
    cap = 3 * slots // (2 * owners)
    padded = owners * cap
    exact = functools.partial(
        jnp.dot, precision=lax.Precision.HIGHEST, preferred_element_type=F32
    )
    own = fold_references(projections, pixels)
    tilt = slot_tilt[0]
    view = slot_view[0, :, 0]
    slot_iota = jnp.arange(slots, dtype=jnp.int32)
    owner_of = view // view_dev
    ahead = (owner_of[:, None] == owner_of[None, :]) & (slot_iota[None, :] < slot_iota[:, None])
    target = owner_of * cap + jnp.sum(ahead.astype(jnp.int32), axis=1)
    matches = (target[None, :] == jnp.arange(padded, dtype=jnp.int32)[:, None]).astype(F32)
    weights = node_weights(slot_pos[0, 0].astype(F32), slot_pos[1, 0].astype(F32), GRID)
    tilt_match = (tilt[:, None] == jnp.arange(tilt_dev, dtype=jnp.int32)[None, :]).astype(F32)
    chosen = exact(tilt_match, warp_grid.reshape(tilt_dev, -1))
    shift_x = jnp.sum(chosen[:, :node_count] * weights, axis=1)
    shift_y = jnp.sum(chosen[:, node_count:] * weights, axis=1)
    facts = jnp.stack(
        [
            slot_iota.astype(F32),
            ((view % view_dev) * tilt_dev + tilt).astype(F32),
            defocus[0].astype(F32),
            shift_x,
            shift_y,
        ],
        axis=1,
    )
    facts = exact(matches, facts)
    src = jnp.round(facts[:, 0]).astype(jnp.int32)
    which = jnp.round(facts[:, 1]).astype(jnp.int32)
    focus = facts[:, 2]
    shifts = facts[:, 3:5]
    meta = jnp.broadcast_to(facts[:, 2:5].T[:, :, None], (3, padded, pixels))
    first, second, nyquist = pass_tables(pixels)
    sums, extra = gather_sums(cap, src, which, own, patches[0], meta, first, second, nyquist)
    terms = exact(finish_terms(sums, extra, focus, shifts, pixels), matches)
    coef = (tilt_match.T[:, None, :] * terms[None, 1:3, :]).reshape(2 * tilt_dev, -1)
    gradient = exact(coef, weights).reshape(tilt_dev, 2 * node_count)
    new_warp = warp_step(gradient, warp_grid.reshape(tilt_dev, 2 * node_count))
    return (terms[:, None, :], new_warp.reshape(warp_grid.shape))


def solution(mesh):
    body = on_device if mesh.shape["rep"] > 1 else on_device_gathered
    in_specs = (
        P(("groups", "tilt"), "dom", None, None),
        P(("groups", "tilt"), "dom", None),
        P(("groups", "tilt"), "dom"),
        P(None, ("groups", "tilt"), "dom"),
        P(("groups", "tilt"), "dom"),
        P(("groups", "dom"), "tilt", None, "rep", None),
        P(("groups", "tilt"), None, None),
    )
    out_specs = (P(None, ("groups", "tilt"), "dom"), P(("groups", "tilt"), None, None))
    return jax.shard_map(
        body, mesh=mesh, in_specs=in_specs, out_specs=out_specs, check_vma=False
    )
```
